512 devices in a mesh: dp: 128 (over y, z, core), feat: 4 (over x).
Axes of the slice: x: 4, y: 8, z: 8, core: 2. Of those that a mesh axis runs over, the one named last changes fastest.
Arguments:
- observations: bfloat16 [16384, 128, 128], P('dp', 'feat'), may hold values from -1.5 to 1.5
- labels: int32 [16384, 128], P('dp'), may hold values 0 or 1
- tile_live: int32 [16384], P('dp'), may hold values from 1 to 128
- tile_group: int32 [16384], P('dp'), may hold values from 0 to 2047, as said below
- position: float32 [2048, 2048], P('dp', 'feat'), may hold values from -2.4 to 2.4
- momentum: float32 [2048, 2048], P('dp', 'feat'), may hold values from -6 to 6
- gradient: float32 [2048, 2048], P('dp', 'feat'), may hold values from -18 to 18
- prior_mean: float32 [2048], P('feat'), may hold values from -1.8 to 1.8
- prior_prec: float32 [128], P('feat'), may hold values from 0.25 to 4
- inv_mass: float32 [128], P('feat'), may hold values from 0.5 to 2
Outputs:
- new_position: float32 [2048, 2048], P('dp', 'feat')
- new_momentum: float32 [2048, 2048], P('dp', 'feat')
- new_gradient: float32 [2048, 2048], P('dp', 'feat')
- energy: float32 [2048, 16], P('dp')
The draws below stay inside these ranges and needn't reach their ends.
Inputs may be any that keep to these rules, and one draw needn't show every extreme that they name: `tile_group`: group g belongs to owner g // 16. Among the 128 tiles of one device at most 2 have groups of any one owner, and one owner has exactly 2 tiles from every device. `tile_live`: the live slots of a tile come first.
All inputs are finite; a program needn't handle non-finite values. No bound on the sum of `labels` on one device may be relied on, other than what follows from the above.
Results may differ from the reference program's by a relative error of at most 0.0041.
Values may be sent and summed in bfloat16 or wider, within the bound.
A program may use at most 64 MiB of HBM per device.

```python
import math
import jax
import jax.numpy as jnp
from jax import lax

F = 128
ROWS = 128
TILE_DEV = 128
GRP_DEV = 16
CHAINS = 16
NTILES = 16384
GROUPS = 2048


def draw_tile_group(key, part):
    owners = GROUPS // GRP_DEV
    block_total = NTILES // TILE_DEV
    slot_count = max(2, 2 * TILE_DEV // owners)
    hot_owner = jax.random.randint(jax.random.fold_in(key, 11), (), 0, owners)
    spare_count = (owners - 1) * slot_count

    def one_block(block_index):
        block_key = jax.random.fold_in(jax.random.fold_in(key, 12), block_index)
        pick_key, order_key, local_key = jax.random.split(block_key, 3)
        candidate = jnp.arange(spare_count, dtype=jnp.int32) // slot_count
        candidate = candidate + (candidate >= hot_owner).astype(jnp.int32)
        chosen = jax.random.permutation(pick_key, candidate)[:TILE_DEV - slot_count]
        target = jnp.concatenate([jnp.full((slot_count,), hot_owner, jnp.int32), chosen.astype(jnp.int32)])
        target = jax.random.permutation(order_key, target)
        local_group = jax.random.randint(local_key, (TILE_DEV,), 0, GRP_DEV)
        return (target * GRP_DEV + local_group).astype(jnp.int32)
    return jax.vmap(one_block)(jnp.arange(block_total, dtype=jnp.int32)).reshape(NTILES).astype(jnp.int32)


def set_ends(drawn, rng, smallest, high):
    shape = drawn.shape
    index_at = [jax.random.randint(jax.random.fold_in(rng, axis), (), 0, shape[axis]) for axis in range(len(shape))]
    drawn = drawn.at[tuple(index_at)].set(smallest)
    longest = shape.index(max(shape))
    index_at[longest] = (index_at[longest] + 1) % shape[longest]
    return drawn.at[tuple(index_at)].set(high)


def block_levels(rng, dims, pieces, low, high):
    loudness = 1.0
    for dim, blocks in pieces:
        draws = jax.random.uniform(jax.random.fold_in(jax.random.fold_in(rng, 6), dim), (blocks,), jnp.float32, low / len(pieces), high / len(pieces))
        loudness = loudness * jnp.repeat(jnp.exp(draws), dims[dim] // blocks).reshape((-1,) + (1,) * (len(dims) - 1 - dim))
    return loudness


def noise(own_key, extent, width, most, pieces=(), kind=jnp.bfloat16):
    factor_of = block_levels(own_key, extent, pieces, -0.22, 0.18) if pieces else 1.0
    result = jax.random.normal(own_key, extent, jnp.float32) * width * factor_of
    return jnp.minimum(jnp.maximum(result, -most), most).astype(kind)


def setup_inputs(seed: int = 0) -> dict:
    arg_keys = jax.random.split(jax.random.key(seed), 11)
    observations = noise(arg_keys[0], (NTILES, F, ROWS), 0.25, 1.5, ((0, 128), (1, 4)))
    labels = set_ends((jax.random.randint(arg_keys[1], (NTILES, ROWS), 0, 2) < 1).astype(jnp.int32), jax.random.fold_in(arg_keys[1], 1), 0, 1)
    tile_live = set_ends(jax.random.randint(arg_keys[2], (NTILES,), 1, ROWS + 1), jax.random.fold_in(arg_keys[2], 1), 1, ROWS).astype(jnp.int32)
    tile_group = draw_tile_group(jax.random.fold_in(arg_keys[10], 71), 0)
    position = noise(arg_keys[4], (GROUPS, F * CHAINS), 0.4, 2.4, ((0, 128), (1, 4)), jnp.float32)
    momentum = noise(arg_keys[5], (GROUPS, F * CHAINS), 1.0, 6.0, ((0, 128), (1, 4)), jnp.float32)
    gradient = noise(arg_keys[6], (GROUPS, F * CHAINS), 3.0, 18.0, ((0, 128), (1, 4)), jnp.float32)
    prior_mean = noise(arg_keys[7], (F * CHAINS,), 0.3, 1.8, ((0, 4),), jnp.float32)
    prior_prec = jnp.clip(jnp.exp(math.log(4.0) - 2.7725887 * jax.random.uniform(arg_keys[8], (F,), jnp.float32) ** block_levels(arg_keys[8], (F,), ((0, 4),), -0.2, 0.2)), 0.25, 4.0)
    inv_mass = jnp.clip(jnp.exp(math.log(2.0) - 1.3862944 * jax.random.uniform(arg_keys[9], (F,), jnp.float32) ** block_levels(arg_keys[9], (F,), ((0, 4),), -0.2, 0.2)), 0.5, 2.0)
    return {"observations": observations, "labels": labels, "tile_live": tile_live, "tile_group": tile_group, "position": position, "momentum": momentum, "gradient": gradient, "prior_mean": prior_mean, "prior_prec": prior_prec, "inv_mass": inv_mass}


step_size = 0.1


def tile_terms(blocks, observations, labels, tile_live):
    logits = jnp.einsum("tfc,tfr->tcr", blocks.astype(jnp.float32), observations.astype(jnp.float32), precision=lax.Precision.HIGHEST)
    live_rows = (jnp.arange(observations.shape[2], dtype=jnp.int32)[None, :] < tile_live[:, None])[:, None, :]
    targets = labels.astype(jnp.float32)[:, None, :]
    residual = jnp.where(live_rows, jax.nn.sigmoid(logits) - targets, 0.0).astype(jnp.bfloat16)
    neg_loglik = jnp.sum(jnp.where(live_rows, jax.nn.softplus(logits) - targets * logits, 0.0), axis=2)
    partial_value = jnp.einsum("tfr,tcr->tfc", observations.astype(jnp.float32), residual.astype(jnp.float32), precision=lax.Precision.HIGHEST)
    return partial_value.reshape(partial_value.shape[0], -1), neg_loglik


def reference(observations, labels, tile_live, tile_group, position, momentum, gradient, prior_mean, prior_prec, inv_mass):
    prior_full = jnp.repeat(prior_prec, CHAINS)
    mass_full = jnp.repeat(inv_mass, CHAINS)
    half_momentum = momentum - 0.5 * step_size * gradient
    moved_position = position + step_size * mass_full * half_momentum
    rounded = moved_position.astype(jnp.bfloat16)
    block_total = NTILES // TILE_DEV

    def one_block(running, block_items):
        tile_obs, tile_labels, live_count, groups = block_items
        blocks = rounded[groups].reshape(groups.shape[0], F, CHAINS)
        partial_value, neg_loglik = tile_terms(blocks, tile_obs, tile_labels, live_count)
        return running, (partial_value, neg_loglik)

    block_items = (observations.reshape(block_total, TILE_DEV, F, ROWS), labels.reshape(block_total, TILE_DEV, ROWS), tile_live.reshape(block_total, TILE_DEV), tile_group.reshape(block_total, TILE_DEV))
    running, outputs = lax.scan(one_block, jnp.zeros((), jnp.float32), block_items)
    partials, losses = outputs
    likelihood_grad = jax.ops.segment_sum(partials.reshape(NTILES, F * CHAINS), tile_group, num_segments=GROUPS)
    group_loglik = jax.ops.segment_sum(losses.reshape(NTILES, CHAINS), tile_group, num_segments=GROUPS)
    offset = moved_position - prior_mean
    new_gradient = likelihood_grad + prior_full * offset
    new_momentum = half_momentum - 0.5 * step_size * new_gradient
    quadratic = 0.5 * (prior_full * offset * offset + mass_full * new_momentum * new_momentum)
    energy = group_loglik + jnp.sum(quadratic.reshape(GROUPS, F, CHAINS), axis=1)
    return moved_position, new_momentum, new_gradient, energy
```

```python
import functools

import jax
import jax.numpy as jnp
from jax import lax
from jax.experimental import pallas as pl
from jax.experimental.pallas import tpu as pltpu
from jax.sharding import PartitionSpec as P

MESH = pl.DeviceIdType.MESH
step_size = 0.1

NY = 8
NC = 2
CHAINS = 16
GRP = 16
LANES = 128
BF = jnp.bfloat16
F32 = jnp.float32


def far_first(n):
    return sorted(range(1, n), key=lambda i: -min(i, n - i))


def dot(a, b, contract=((1,), (0,))):
    return lax.dot_general(a, b, (contract, ((), ())), preferred_element_type=F32)


def one_hot(flags):
    return jnp.where(flags, 1.0, 0.0).astype(BF)


def kernel(
    obs,
    lab,
    live,
    tg,
    pos,
    mom,
    grd,
    pm,
    pp,
    im,
    new_pos,
    new_mom,
    new_grd,
    energy,
    obsx,
    perm,
    labf,
    mask,
    half_s,
    ltile,
    gat,
    rqs,
    rq,
    tmat,
    tmat_t,
    smat,
    smat_t,
    sels,
    selr,
    xs,
    xr,
    gs,
    gr,
    wf,
    gf,
    ms,
    mr,
    ys,
    yr,
    er,
    obs_ss,
    obs_rs,
    own_s,
    gat_ss,
    gat_rs,
    rq_ss,
    rq_rs,
    sel_ss,
    sel_rs,
    x_ss,
    x_rs,
    gx_ss,
    gx_rs,
    m_ss,
    m_rs,
    y_ss,
    y_rs,
    e_ss,
    e_rs,
):
    d = lax.axis_index("dp")
    k = lax.axis_index("feat")
    y, z, c = d // (NY * NC), (d // NC) % NY, d % NC
    tiles = lab.shape[0]
    nf = 4
    share = tiles // nf
    width = pos.shape[1]
    quarter = width // CHAINS
    half_w = width // 2

    def at(yy, zz, cc):
        return ((yy * NY + zz) * NC + cc, k)

    def xpeer(i):
        return (d, (k + i) % nf)

    g_me = (y, z)
    s_me = (z * NC + c, y * NC + c)

    def g_peer(a, i):
        return at((y + i) % NY, z, c) if a == 0 else at(y, (z + i) % NY, c)

    def s_peer(a, i):
        q = (s_me[a] + i) % (NY * NC)
        return at(y, q // NC, q % NC) if a == 0 else at(q // NC, z, q % NC)

    x_order = (2, 1, 3)
    g_order = far_first(NY)
    s_order = far_first(NY * NC)

    barrier = pltpu.get_barrier_semaphore()
    count = 0
    for i in x_order:
        pl.semaphore_signal(barrier, inc=1, device_id=xpeer(i), device_id_type=MESH)
        count += 1
    for zz in range(NY):
        for cc in range(NC):
            if (zz, cc) != (0, 0):
                who = at(y, (z + zz) % NY, (c + cc) % NC)
                pl.semaphore_signal(barrier, inc=1, device_id=who, device_id_type=MESH)
                count += 1
            if zz != 0:
                who = at((y + zz) % NY, z, (c + cc) % NC)
                pl.semaphore_signal(barrier, inc=1, device_id=who, device_id_type=MESH)
                count += 1

    src = lax.broadcasted_iota(jnp.int32, (LANES, width), 0)
    dst = lax.broadcasted_iota(jnp.int32, (LANES, width), 1)
    want = (dst % quarter) * CHAINS + dst // quarter
    for b in range(width // LANES):
        perm[b * LANES : (b + 1) * LANES, :] = one_hot(src + b * LANES == want)

    half = mom[...] - 0.5 * step_size * grd[...]
    moved = pos[...] + step_size * im[...] * half
    half_s[...] = half
    new_pos[...] = moved
    block = dot(moved.astype(BF), perm[...]).astype(BF)
    for a in range(2):
        gat[a, pl.ds(g_me[a], 1)] = block[None, :, a * half_w : (a + 1) * half_w]

    tile_row = jnp.broadcast_to(tg[...], (tiles, tiles))
    tile_col = jnp.transpose(tile_row.astype(F32)).astype(jnp.int32)
    own_row, own_col = tile_row // GRP, tile_col // GRP
    t_row = lax.broadcasted_iota(jnp.int32, (tiles, tiles), 1)
    t_col = lax.broadcasted_iota(jnp.int32, (tiles, tiles), 0)
    same = own_row == own_col
    rank_row = jnp.sum(jnp.where(same & (t_col < t_row), 1.0, 0.0), axis=0, keepdims=True)
    rank_row = jnp.broadcast_to(rank_row, (tiles, tiles))
    rank_col = jnp.transpose(rank_row).astype(jnp.int32)
    rank_row = rank_row.astype(jnp.int32)
    slots = NY * NC * NY * 2

    def slot_of(a, own, rank):
        oy, oz, oc = own // (NY * NC), (own // NC) % NY, own % NC
        first, second = (oy, oz) if a == 0 else (oz, oy)
        return (second * NC + oc) * (NY * 2) + first * 2 + rank, first

    for a in range(2):
        s_r, _ = slot_of(a, own_row, rank_row)
        s_c, first = slot_of(a, own_col, rank_col)
        asked = (first * GRP + tile_col % GRP + 1).astype(F32).astype(BF)
        for b in range(slots // LANES):
            tmat[a, :, b * LANES : (b + 1) * LANES] = one_hot(s_c == t_row + b * LANES)
            tmat_t[a, b * LANES : (b + 1) * LANES, :] = one_hot(s_r == t_col + b * LANES)
        rqs[a] = dot(tmat_t[a], asked).astype(BF).reshape(NY * NC, NY * 2, LANES)

    pl.semaphore_wait(barrier, count)

    copies = []

    def send(src_ref, dst_ref, ss, rs, who):
        copy = pltpu.make_async_remote_copy(
            src_ref=src_ref, dst_ref=dst_ref, send_sem=ss, recv_sem=rs, device_id=who, device_id_type=MESH
        )
        copy.start()
        copies.append(copy)
        return copy

    gat_c = [[], []]
    rq_c = [[], []]
    for a in range(2):
        for i in g_order:
            ref = gat.at[a, g_me[a]]
            gat_c[a].append(send(ref, ref, gat_ss.at[a, i], gat_rs.at[a, i], g_peer(a, i)))
    for a in range(2):
        for i in s_order:
            q = (s_me[a] + i) % (NY * NC)
            rq_c[a].append(send(rqs.at[a, q], rq.at[a, s_me[a]], rq_ss.at[a, i], rq_rs.at[a, i], s_peer(a, i)))
    obs_c = []
    for i in x_order:
        to = (k + i) % nf
        obs_c.append(
            send(
                obs.at[pl.ds(to * share, share)],
                obsx.at[:, pl.ds(pl.multiple_of(k * quarter, quarter), quarter), :],
                obs_ss.at[i],
                obs_rs.at[i],
                xpeer(i),
            )
        )
    own_copy = pltpu.make_async_copy(
        obs.at[pl.ds(k * share, share)],
        obsx.at[:, pl.ds(pl.multiple_of(k * quarter, quarter), quarter), :],
        own_s,
    )
    own_copy.start()

    rows = pl.ds(pl.multiple_of(k * share, share), share)
    labf[...] = lab[rows, :].astype(F32)
    live_col = jnp.transpose(jnp.broadcast_to(live[...], (tiles, tiles)).astype(F32))
    mask[...] = jnp.where(t_row.astype(F32) < live_col, 1.0, 0.0)
    ltile[...] = jnp.zeros_like(ltile)

    for a in range(2):
        rq[a, pl.ds(s_me[a], 1)] = rqs[a, pl.ds(s_me[a], 1)]
        for copy in rq_c[a]:
            copy.wait_recv()
        ask = rq[a].reshape(slots, LANES).astype(F32)
        lane1 = (lax.broadcasted_iota(jnp.int32, (slots, LANES), 1) + 1).astype(F32)
        chosen = jnp.where(ask == lane1, 1.0, 0.0)
        smat[a] = chosen.astype(BF)
        for b in range(slots // LANES):
            smat_t[a, :, b * LANES : (b + 1) * LANES] = jnp.transpose(
                chosen[b * LANES : (b + 1) * LANES, :]
            ).astype(BF)

    sel_c = [[], []]
    for a in range(2):
        for copy in gat_c[a]:
            copy.wait_recv()
        table = gat[a].reshape(NY * GRP, half_w)
        sels[a] = dot(smat[a], table).astype(BF).reshape(NY * NC, NY * 2, half_w)
        for i in s_order:
            q = (s_me[a] + i) % (NY * NC)
            sel_c[a].append(
                send(sels.at[a, q], selr.at[a, s_me[a]], sel_ss.at[a, i], sel_rs.at[a, i], s_peer(a, i))
            )
        selr[a, pl.ds(s_me[a], 1)] = sels[a, pl.ds(s_me[a], 1)]

    x_c = [[], []]
    for a in range(2):
        for copy in sel_c[a]:
            copy.wait_recv()
        rows_a = dot(tmat[a], selr[a].reshape(slots, half_w)).astype(BF)
        xs[a] = rows_a.reshape(nf, share, half_w)
        for i in x_order:
            to = (k + i) % nf
            x_c[a].append(send(xs.at[a, to], xr.at[a, k], x_ss.at[a, i], x_rs.at[a, i], xpeer(i)))
        xr[a, pl.ds(k, 1)] = xs[a, pl.ds(k, 1)]

    lane = lax.broadcasted_iota(jnp.int32, (share, LANES), 1) // quarter
    per = LANES // quarter
    for a in range(2):
        for copy in x_c[a]:
            copy.wait_recv()
        for b in range(half_w // LANES):
            came = [xr[a, kk, :, b * LANES : (b + 1) * LANES].astype(F32) for kk in range(nf)]
            for ci in range(per):
                out = jnp.zeros((share, LANES), F32)
                for kk in range(nf):
                    shift = ((kk - ci) * quarter) % LANES
                    moved_k = came[kk] if shift == 0 else pltpu.roll(came[kk], shift, 1)
                    out = jnp.where(lane == kk, moved_k, out)
                chain = a * (CHAINS // 2) + b * per + ci
                wf[chain * share : (chain + 1) * share, :] = out

    own_copy.wait()
    for copy in obs_c:
        copy.wait_recv()

    lane16 = lax.broadcasted_iota(jnp.int32, (CHAINS, LANES), 1)
    loglik = jnp.zeros((CHAINS, LANES), F32)
    base = k * share
    for t in range(share):
        coeff = wf[pl.ds(t, CHAINS, stride=share), :].astype(BF)
        tile = obsx[t]
        logits = dot(coeff, tile)
        target = jnp.broadcast_to(labf[t : t + 1, :], (CHAINS, LANES))
        alive = jnp.broadcast_to(mask[pl.ds(base + t, 1), :], (CHAINS, LANES)) > 0.5
        e = jnp.exp(-jnp.abs(logits))
        r = 1.0 / (1.0 + e)
        sig = jnp.where(logits >= 0.0, r, e * r)
        residual = jnp.where(alive, sig - target, 0.0).astype(BF)
        soft = jnp.maximum(logits, 0.0) + jnp.log1p(e)
        term = jnp.where(alive, soft - target * logits, 0.0)
        loglik = jnp.where(lane16 == t, jnp.sum(term, axis=1, keepdims=True), loglik)
        gf[pl.ds(t, CHAINS, stride=share), :] = dot(residual, tile, ((1,), (1,)))

    gx_c = [[], []]
    for a in range(2):
        for b in range(half_w // LANES):
            chain = a * (CHAINS // 2) + b * per
            made = [gf[(chain + ci) * share : (chain + ci + 1) * share, :] for ci in range(per)]
            for kk in range(nf):
                out = jnp.zeros((share, LANES), F32)
                for ci in range(per):
                    shift = ((ci - kk) * quarter) % LANES
                    moved_c = made[ci] if shift == 0 else pltpu.roll(made[ci], shift, 1)
                    out = jnp.where(lane == ci, moved_c, out)
                gs[a, kk, :, b * LANES : (b + 1) * LANES] = out.astype(BF)
        for i in x_order:
            to = (k + i) % nf
            gx_c[a].append(send(gs.at[a, to], gr.at[a, k], gx_ss.at[a, i], gx_rs.at[a, i], xpeer(i)))
        gr[a, pl.ds(k, 1)] = gs[a, pl.ds(k, 1)]

    high = loglik.astype(BF).astype(F32)
    both = jnp.concatenate([high, loglik - high, jnp.zeros((LANES - 2 * CHAINS, LANES), F32)], axis=0)
    ltile[rows, :] = jnp.transpose(both)[:share, :].astype(BF)

    m_c = [[], []]
    for a in range(2):
        for copy in gx_c[a]:
            copy.wait_recv()
        sent = dot(tmat_t[a], gr[a].reshape(tiles, half_w)).astype(BF)
        ms[a, :, :, :half_w] = sent.reshape(NY * NC, NY * 2, half_w)
        w = half_w
        if a == 0:
            ext = dot(tmat_t[a], ltile[...]).astype(BF)
            ms[a, :, :, half_w:] = ext.reshape(NY * NC, NY * 2, LANES)
            w = half_w + LANES
        for i in s_order:
            q = (s_me[a] + i) % (NY * NC)
            m_c[a].append(
                send(
                    ms.at[a, q, :, pl.ds(0, w)],
                    mr.at[a, s_me[a], :, pl.ds(0, w)],
                    m_ss.at[a, i],
                    m_rs.at[a, i],
                    s_peer(a, i),
                )
            )
        mr[a, pl.ds(s_me[a], 1), :, :w] = ms[a, pl.ds(s_me[a], 1), :, :w]

    y_c = [[], []]
    for a in range(2):
        w = half_w + LANES if a == 0 else half_w
        for copy in m_c[a]:
            copy.wait_recv()
        summed = dot(smat_t[a], mr[a, :, :, :w].reshape(slots, w)).astype(BF)
        ys[a, :, :, :w] = summed.reshape(NY, GRP, w)
        for i in g_order:
            to = (g_me[a] + i) % NY
            y_c[a].append(
                send(
                    ys.at[a, to, :, pl.ds(0, w)],
                    yr.at[a, g_me[a], :, pl.ds(0, w)],
                    y_ss.at[a, i],
                    y_rs.at[a, i],
                    g_peer(a, i),
                )
            )
        yr[a, pl.ds(g_me[a], 1), :, :w] = ys[a, pl.ds(g_me[a], 1), :, :w]

    lik = jnp.zeros((GRP, width), F32)
    group_loglik = jnp.zeros((GRP, LANES), F32)
    for a in range(2):
        for copy in y_c[a]:
            copy.wait_recv()
        part = yr[a, :, :, :half_w].reshape(NY * GRP, half_w)
        back = dot(part, perm[:, a * half_w : (a + 1) * half_w], ((1,), (1,)))
        for g in range(NY):
            lik = lik + back[g * GRP : (g + 1) * GRP, :]
        if a == 0:
            for g in range(NY):
                group_loglik = group_loglik + yr[a, g, :, half_w:].astype(F32)

    offset = new_pos[...] - pm[...]
    grad_now = lik + pp[...] * offset
    mom_now = half_s[...] - 0.5 * step_size * grad_now
    new_grd[...] = grad_now
    new_mom[...] = mom_now
    quad = 0.5 * (pp[...] * offset * offset + im[...] * mom_now * mom_now)
    total = quad[:, :LANES]
    for b in range(1, width // LANES):
        total = total + quad[:, b * LANES : (b + 1) * LANES]
    shift = LANES // 2
    while shift >= CHAINS:
        total = total + pltpu.roll(total, shift, 1)
        shift //= 2
    total = total + group_loglik + pltpu.roll(group_loglik, LANES - CHAINS, 1)
    er[pl.ds(k, 1)] = total[None]
    e_c = []
    for i in x_order:
        e_c.append(send(er.at[k], er.at[k], e_ss.at[i], e_rs.at[i], xpeer(i)))
    for copy in e_c:
        copy.wait_recv()
    whole = er[0]
    for kk in range(1, nf):
        whole = whole + er[kk]
    energy[...] = whole[:, :CHAINS]
    for copy in copies:
        copy.wait_send()


def body(observations, labels, tile_live, tile_group, position, momentum, gradient, prior_mean, prior_prec, inv_mass):
    tiles, quarter, row_count = observations.shape
    groups, width = position.shape
    chains = width // quarter
    nf = lax.axis_size("feat")
    half_w = width // 2
    share = tiles // nf
    S = NY * NC
    prior_full = jnp.repeat(prior_prec, chains)[None, :]
    mass_full = jnp.repeat(inv_mass, chains)[None, :]
    V = pltpu.VMEM
    D = pltpu.SemaphoreType.DMA
    scratch = [
        V((share, nf * quarter, row_count), BF),
        V((width, width), BF),
        V((share, row_count), F32),
        V((tiles, LANES), F32),
        V((groups, width), F32),
        V((tiles, LANES), BF),
        V((2, NY, GRP, half_w), BF),
        V((2, S, 2 * NY, LANES), BF),
        V((2, S, 2 * NY, LANES), BF),
        V((2, tiles, S * 2 * NY), BF),
        V((2, S * 2 * NY, tiles), BF),
        V((2, S * 2 * NY, LANES), BF),
        V((2, LANES, S * 2 * NY), BF),
        V((2, S, 2 * NY, half_w), BF),
        V((2, S, 2 * NY, half_w), BF),
        V((2, nf, share, half_w), BF),
        V((2, nf, share, half_w), BF),
        V((2, nf, share, half_w), BF),
        V((2, nf, share, half_w), BF),
        V((CHAINS * share, LANES), F32),
        V((CHAINS * share, LANES), F32),
        V((2, S, 2 * NY, half_w + LANES), BF),
        V((2, S, 2 * NY, half_w + LANES), BF),
        V((2, NY, GRP, half_w + LANES), BF),
        V((2, NY, GRP, half_w + LANES), BF),
        V((nf, groups, LANES), F32),
        D((nf,)),
        D((nf,)),
        D(()),
        D((2, NY)),
        D((2, NY)),
        D((2, S)),
        D((2, S)),
        D((2, S)),
        D((2, S)),
        D((2, nf)),
        D((2, nf)),
        D((2, nf)),
        D((2, nf)),
        D((2, S)),
        D((2, S)),
        D((2, NY)),
        D((2, NY)),
        D((nf,)),
        D((nf,)),
    ]
    vm = pl.BlockSpec(memory_space=pltpu.VMEM)
    moved, new_mom, new_grd, energy = pl.pallas_call(
        kernel,
        out_shape=(
            jax.ShapeDtypeStruct((groups, width), F32),
            jax.ShapeDtypeStruct((groups, width), F32),
            jax.ShapeDtypeStruct((groups, width), F32),
            jax.ShapeDtypeStruct((groups, chains), F32),
        ),
        in_specs=[pl.BlockSpec(memory_space=pl.ANY)] + [vm] * 9,
        out_specs=(vm, vm, vm, vm),
        scratch_shapes=scratch,
        compiler_params=pltpu.CompilerParams(collective_id=0, has_side_effects=True),
        name="leapfrog",
    )(
        observations,
        labels,
        tile_live[None, :],
        tile_group[None, :],
        position,
        momentum,
        gradient,
        prior_mean[None, :],
        prior_full,
        mass_full,
    )
    return moved, new_mom, new_grd, energy


def solution(mesh):
    placed = (
        P("dp", "feat", None),
        P("dp", None),
        P("dp"),
        P("dp"),
        P("dp", "feat"),
        P("dp", "feat"),
        P("dp", "feat"),
        P("feat"),
        P("feat"),
        P("feat"),
    )
    return jax.shard_map(
        body,
        mesh=mesh,
        in_specs=placed,
        out_specs=(P("dp", "feat"), P("dp", "feat"), P("dp", "feat"), P("dp", None)),
        check_vma=False,
    )
```

```python
import functools

import jax
import jax.numpy as jnp
from jax import lax
from jax.experimental import pallas as pl
from jax.experimental.pallas import tpu as pltpu
from jax.sharding import PartitionSpec as P

MESH = pl.DeviceIdType.MESH
step_size = 0.1

NY = 8
NC = 2
CHAINS = 16
GRP = 16
LANES = 128
BF = jnp.bfloat16
F32 = jnp.float32


def far_first(n):
    return sorted(range(1, n), key=lambda i: -min(i, n - i))


def dot(a, b, contract=((1,), (0,))):
    return lax.dot_general(a, b, (contract, ((), ())), preferred_element_type=F32)


def one_hot(flags):
    return jnp.where(flags, 1.0, 0.0).astype(BF)


def kernel(
    obs,
    lab_h,
    live_h,
    tg_h,
    pos_h,
    mom_h,
    grd_h,
    pm_h,
    pp_h,
    im_h,
    new_pos,
    new_mom,
    new_grd,
    energy,
    lab,
    live,
    tg,
    pos,
    mom,
    grd,
    pm,
    ppim_p,
    ppim_m,
    in_s,
    obsx,
    perm,
    labf,
    mask,
    half_s,
    ltile,
    gat,
    rqs,
    rq,
    fold,
    tmat,
    tmat_t,
    smat,
    smat_t,
    sels,
    selr,
    xs,
    xr,
    gs,
    gr,
    wf,
    gf,
    lg,
    res,
    ms,
    mr,
    ys,
    yr,
    er,
    obs_ss,
    obs_rs,
    own_s,
    gat_ss,
    gat_rs,
    rq_ss,
    rq_rs,
    sel_ss,
    sel_rs,
    x_ss,
    x_rs,
    gx_ss,
    gx_rs,
    m_ss,
    m_rs,
    y_ss,
    y_rs,
    e_ss,
    e_rs,
):
    d = lax.axis_index("dp")
    k = lax.axis_index("feat")
    y, z, c = d // (NY * NC), (d // NC) % NY, d % NC
    tiles = lab_h.shape[0]
    nf = 4
    share = tiles // nf
    width = pos_h.shape[1]
    quarter = width // CHAINS
    half_w = width // 2

    def at(yy, zz, cc):
        return ((yy * NY + zz) * NC + cc, k)

    def xpeer(i):
        return (d, (k + i) % nf)

    g_me = (y, z)
    s_me = (z * NC + c, y * NC + c)

    def g_peer(a, i):
        return at((y + i) % NY, z, c) if a == 0 else at(y, (z + i) % NY, c)

    def s_peer(a, i):
        q = (s_me[a] + i) % (NY * NC)
        return at(y, q // NC, q % NC) if a == 0 else at(q // NC, z, q % NC)

    x_order = (2, 1, 3)
    g_order = far_first(NY)
    s_order = far_first(NY * NC)

    barrier = pltpu.get_barrier_semaphore()
    count = 0
    for i in x_order:
        pl.semaphore_signal(barrier, inc=1, device_id=xpeer(i), device_id_type=MESH)
        count += 1
    for zz in range(NY):
        for cc in range(NC):
            if (zz, cc) != (0, 0):
                who = at(y, (z + zz) % NY, (c + cc) % NC)
                pl.semaphore_signal(barrier, inc=1, device_id=who, device_id_type=MESH)
                count += 1
            if zz != 0:
                who = at((y + zz) % NY, z, (c + cc) % NC)
                pl.semaphore_signal(barrier, inc=1, device_id=who, device_id_type=MESH)
                count += 1

    loads = []
    for i, (far, near) in enumerate(
        (
            (tg_h, tg),
            (pp_h, ppim_p),
            (im_h, ppim_m),
            (pos_h, pos),
            (mom_h, mom),
            (grd_h, grd),
            (pm_h, pm),
            (live_h, live),
            (lab_h, lab),
        )
    ):
        loads.append(pltpu.make_async_copy(far, near, in_s.at[i]))
        loads[-1].start()

    src = lax.broadcasted_iota(jnp.int32, (LANES, width), 0)
    dst = lax.broadcasted_iota(jnp.int32, (LANES, width), 1)
    want = (dst % quarter) * CHAINS + dst // quarter
    for b in range(width // LANES):
        perm[b * LANES : (b + 1) * LANES, :] = one_hot(src + b * LANES == want)

    for copy in loads[1:7]:
        copy.wait()
    row8 = lax.broadcasted_iota(jnp.int32, (8, quarter), 0)
    pieces = jnp.zeros((8, quarter), F32)
    for n, ref in enumerate((ppim_p, ppim_m)):
        rest = ref[...]
        for m in range(3):
            piece = rest.astype(BF).astype(F32)
            pieces = jnp.where(row8 == 3 * n + m, piece, pieces)
            rest = rest - piece
    feature = lax.broadcasted_iota(jnp.int32, (quarter, width), 0)
    chain_lane = lax.broadcasted_iota(jnp.int32, (quarter, width), 1)
    spread = dot(pieces.astype(BF), one_hot(chain_lane // CHAINS == feature))
    pp = (spread[0:1, :] + spread[1:2, :]) + spread[2:3, :]
    im = (spread[3:4, :] + spread[4:5, :]) + spread[5:6, :]

    half = mom[...] - 0.5 * step_size * grd[...]
    moved = pos[...] + step_size * im * half
    half_s[...] = half
    new_pos[...] = moved
    block = dot(moved.astype(BF), perm[...]).astype(BF)
    for a in range(2):
        gat[a, pl.ds(g_me[a], 1)] = block[None, :, a * half_w : (a + 1) * half_w]

    loads[0].wait()
    tile_row = jnp.broadcast_to(tg[...], (tiles, tiles))
    tile_col = jnp.transpose(tile_row.astype(F32)).astype(jnp.int32)
    own_row, own_col = tile_row // GRP, tile_col // GRP
    t_row = lax.broadcasted_iota(jnp.int32, (tiles, tiles), 1)
    t_col = lax.broadcasted_iota(jnp.int32, (tiles, tiles), 0)
    same = own_row == own_col
    rank_row = jnp.sum(jnp.where(same & (t_col < t_row), 1.0, 0.0), axis=0, keepdims=True)
    rank_row = jnp.broadcast_to(rank_row, (tiles, tiles))
    rank_col = jnp.transpose(rank_row).astype(jnp.int32)
    rank_row = rank_row.astype(jnp.int32)
    slots = NY * NC * NY * 2

    def slot_of(a, own, rank):
        oy, oz, oc = own // (NY * NC), (own // NC) % NY, own % NC
        first, second = (oy, oz) if a == 0 else (oz, oy)
        return (second * NC + oc) * (NY * 2) + first * 2 + rank, first

    for a in range(2):
        s_r, first = slot_of(a, own_row, rank_row)
        asked = (first * GRP + tile_row % GRP + 1)[:16, :].astype(F32).astype(BF)
        s_c, _ = slot_of(a, own_col, rank_col)
        for b in range(slots // LANES):
            tmat[a, :, b * LANES : (b + 1) * LANES] = one_hot(s_c == t_row + b * LANES)
            tmat_t[a, b * LANES : (b + 1) * LANES, :] = one_hot(s_r == t_col + b * LANES)
        rqs[a] = dot(asked, tmat[a])[:1, :]

    pl.semaphore_wait(barrier, count)

    copies = []

    def send(src_ref, dst_ref, ss, rs, who):
        copy = pltpu.make_async_remote_copy(
            src_ref=src_ref, dst_ref=dst_ref, send_sem=ss, recv_sem=rs, device_id=who, device_id_type=MESH
        )
        copy.start()
        copies.append(copy)
        return copy

    gat_c = [[], []]
    rq_c = [[], []]
    for a in range(2):
        for i in s_order:
            rq_c[a].append(send(rqs.at[a], rq.at[a, s_me[a]], rq_ss.at[a, i], rq_rs.at[a, i], s_peer(a, i)))
    for a in range(2):
        for i in g_order:
            ref = gat.at[a, g_me[a]]
            gat_c[a].append(send(ref, ref, gat_ss.at[a, i], gat_rs.at[a, i], g_peer(a, i)))
    obs_c = []
    for i in x_order:
        to = (k + i) % nf
        obs_c.append(
            send(
                obs.at[pl.ds(to * share, share)],
                obsx.at[:, pl.ds(pl.multiple_of(k * quarter, quarter), quarter), :],
                obs_ss.at[i],
                obs_rs.at[i],
                xpeer(i),
            )
        )
    own_copy = pltpu.make_async_copy(
        obs.at[pl.ds(k * share, share)],
        obsx.at[:, pl.ds(pl.multiple_of(k * quarter, quarter), quarter), :],
        own_s,
    )
    own_copy.start()

    loads[7].wait()
    loads[8].wait()
    rows = pl.ds(pl.multiple_of(k * share, share), share)
    labf[...] = lab[rows, :].astype(F32)
    live_col = jnp.transpose(jnp.broadcast_to(live[...], (tiles, tiles)).astype(F32))
    mask[...] = jnp.where(t_row.astype(F32) < live_col, 1.0, 0.0)
    ltile[...] = jnp.zeros_like(ltile)
    for b in range(slots // LANES):
        here = lax.broadcasted_iota(jnp.int32, (LANES, slots), 0) + b * LANES
        there = lax.broadcasted_iota(jnp.int32, (LANES, slots), 1)
        fold[b * LANES : (b + 1) * LANES, :] = one_hot(here % (NY * 2) == there % (NY * 2))

    lane_q = lax.broadcasted_iota(jnp.int32, (NY * NC, slots), 1) // (NY * 2)
    row_q = lax.broadcasted_iota(jnp.int32, (NY * NC, slots), 0)
    for a in range(2):
        rq[a, pl.ds(s_me[a], 1)] = rqs[a][None]
        for copy in rq_c[a]:
            copy.wait_recv()
        asks = jnp.where(lane_q == s_me[a], rq[a].reshape(NY * NC, slots), 0.0).astype(BF)
        asks = jnp.where(lane_q == row_q, dot(asks, fold[...]), 0.0)
        ask = jnp.sum(asks, axis=0, keepdims=True)
        for b in range(slots // LANES):
            part = jnp.broadcast_to(ask[:, b * LANES : (b + 1) * LANES], (LANES, LANES))
            chosen = jnp.where(part == (t_col + 1).astype(F32), 1.0, 0.0)
            smat_t[a, :, b * LANES : (b + 1) * LANES] = chosen.astype(BF)
            smat[a, b * LANES : (b + 1) * LANES, :] = jnp.transpose(chosen).astype(BF)

    sel_c = [[], []]
    for a in range(2):
        for copy in gat_c[a]:
            copy.wait_recv()
        table = gat[a].reshape(NY * GRP, half_w)
        sels[a] = dot(smat[a], table).astype(BF).reshape(NY * NC, NY * 2, half_w)
        for i in s_order:
            q = (s_me[a] + i) % (NY * NC)
            sel_c[a].append(
                send(sels.at[a, q], selr.at[a, s_me[a]], sel_ss.at[a, i], sel_rs.at[a, i], s_peer(a, i))
            )
        selr[a, pl.ds(s_me[a], 1)] = sels[a, pl.ds(s_me[a], 1)]

    x_c = [[], []]
    for a in range(2):
        for copy in sel_c[a]:
            copy.wait_recv()
        rows_a = dot(tmat[a], selr[a].reshape(slots, half_w)).astype(BF)
        xs[a] = rows_a.reshape(nf, share, half_w)
        for i in x_order:
            to = (k + i) % nf
            x_c[a].append(send(xs.at[a, to], xr.at[a, k], x_ss.at[a, i], x_rs.at[a, i], xpeer(i)))
        xr[a, pl.ds(k, 1)] = xs[a, pl.ds(k, 1)]

    lane = lax.broadcasted_iota(jnp.int32, (share, LANES), 1) // quarter
    per = LANES // quarter
    for a in range(2):
        for copy in x_c[a]:
            copy.wait_recv()
        for b in range(half_w // LANES):
            came = [xr[a, kk, :, b * LANES : (b + 1) * LANES].astype(F32) for kk in range(nf)]
            for ci in range(per):
                out = jnp.zeros((share, LANES), F32)
                for kk in range(nf):
                    shift = ((kk - ci) * quarter) % LANES
                    moved_k = came[kk] if shift == 0 else pltpu.roll(came[kk], shift, 1)
                    out = jnp.where(lane == kk, moved_k, out)
                chain = a * (CHAINS // 2) + b * per + ci
                wf[chain * share : (chain + 1) * share, :] = out

    own_copy.wait()
    for copy in obs_c:
        copy.wait_recv()

    lane16 = lax.broadcasted_iota(jnp.int32, (CHAINS, LANES), 1)
    loglik = jnp.zeros((CHAINS, LANES), F32)
    base = k * share
    for t in range(share):
        coeff = wf[pl.ds(t, CHAINS, stride=share), :].astype(BF)
        lg[t * CHAINS : (t + 1) * CHAINS, :] = dot(coeff, obsx[t])
    for t in range(share):
        logits = lg[t * CHAINS : (t + 1) * CHAINS, :]
        target = jnp.broadcast_to(labf[t : t + 1, :], (CHAINS, LANES))
        alive = jnp.broadcast_to(mask[pl.ds(base + t, 1), :], (CHAINS, LANES)) > 0.5
        e = jnp.exp(-jnp.abs(logits))
        r = 1.0 / (1.0 + e)
        sig = jnp.where(logits >= 0.0, r, e * r)
        res[t * CHAINS : (t + 1) * CHAINS, :] = jnp.where(alive, sig - target, 0.0).astype(BF)
        soft = jnp.maximum(logits, 0.0) + jnp.log1p(e)
        term = jnp.where(alive, soft - target * logits, 0.0)
        loglik = jnp.where(lane16 == t, jnp.sum(term, axis=1, keepdims=True), loglik)
    for t in range(share):
        gf[pl.ds(t, CHAINS, stride=share), :] = dot(res[t * CHAINS : (t + 1) * CHAINS, :], obsx[t], ((1,), (1,)))

    gx_c = [[], []]
    for a in range(2):
        for b in range(half_w // LANES):
            chain = a * (CHAINS // 2) + b * per
            made = [gf[(chain + ci) * share : (chain + ci + 1) * share, :] for ci in range(per)]
            for kk in range(nf):
                out = jnp.zeros((share, LANES), F32)
                for ci in range(per):
                    shift = ((ci - kk) * quarter) % LANES
                    moved_c = made[ci] if shift == 0 else pltpu.roll(made[ci], shift, 1)
                    out = jnp.where(lane == ci, moved_c, out)
                gs[a, kk, :, b * LANES : (b + 1) * LANES] = out.astype(BF)
        for i in x_order:
            to = (k + i) % nf
            gx_c[a].append(send(gs.at[a, to], gr.at[a, k], gx_ss.at[a, i], gx_rs.at[a, i], xpeer(i)))
        gr[a, pl.ds(k, 1)] = gs[a, pl.ds(k, 1)]

    high = loglik.astype(BF).astype(F32)
    both = jnp.concatenate([high, loglik - high, jnp.zeros((LANES - 2 * CHAINS, LANES), F32)], axis=0)
    ltile[rows, :] = jnp.transpose(both)[:share, :].astype(BF)

    m_c = [[], []]
    for a in range(2):
        for copy in gx_c[a]:
            copy.wait_recv()
        sent = dot(tmat_t[a], gr[a].reshape(tiles, half_w)).astype(BF)
        ms[a, :, :, :half_w] = sent.reshape(NY * NC, NY * 2, half_w)
        w = half_w
        if a == 0:
            ext = dot(tmat_t[a], ltile[...]).astype(BF)
            ms[a, :, :, half_w:] = ext.reshape(NY * NC, NY * 2, LANES)
            w = half_w + LANES
        for i in s_order:
            q = (s_me[a] + i) % (NY * NC)
            m_c[a].append(
                send(
                    ms.at[a, q, :, pl.ds(0, w)],
                    mr.at[a, s_me[a], :, pl.ds(0, w)],
                    m_ss.at[a, i],
                    m_rs.at[a, i],
                    s_peer(a, i),
                )
            )
        mr[a, pl.ds(s_me[a], 1), :, :w] = ms[a, pl.ds(s_me[a], 1), :, :w]

    y_c = [[], []]
    for a in range(2):
        w = half_w + LANES if a == 0 else half_w
        for copy in m_c[a]:
            copy.wait_recv()
        summed = dot(smat_t[a], mr[a, :, :, :w].reshape(slots, w)).astype(BF)
        ys[a, :, :, :w] = summed.reshape(NY, GRP, w)
        for i in g_order:
            to = (g_me[a] + i) % NY
            y_c[a].append(
                send(
                    ys.at[a, to, :, pl.ds(0, w)],
                    yr.at[a, g_me[a], :, pl.ds(0, w)],
                    y_ss.at[a, i],
                    y_rs.at[a, i],
                    g_peer(a, i),
                )
            )
        yr[a, pl.ds(g_me[a], 1), :, :w] = ys[a, pl.ds(g_me[a], 1), :, :w]

    lik = jnp.zeros((GRP, width), F32)
    group_loglik = jnp.zeros((GRP, LANES), F32)
    for a in range(2):
        for copy in y_c[a]:
            copy.wait_recv()
        part = yr[a, :, :, :half_w].reshape(NY * GRP, half_w)
        back = dot(part, perm[:, a * half_w : (a + 1) * half_w], ((1,), (1,)))
        for g in range(NY):
            lik = lik + back[g * GRP : (g + 1) * GRP, :]
        if a == 0:
            for g in range(NY):
                group_loglik = group_loglik + yr[a, g, :, half_w:].astype(F32)

    offset = new_pos[...] - pm[...]
    grad_now = lik + pp * offset
    mom_now = half_s[...] - 0.5 * step_size * grad_now
    new_grd[...] = grad_now
    new_mom[...] = mom_now
    quad = 0.5 * (pp * offset * offset + im * mom_now * mom_now)
    total = quad[:, :LANES]
    for b in range(1, width // LANES):
        total = total + quad[:, b * LANES : (b + 1) * LANES]
    shift = LANES // 2
    while shift >= CHAINS:
        total = total + pltpu.roll(total, shift, 1)
        shift //= 2
    total = total + group_loglik + pltpu.roll(group_loglik, LANES - CHAINS, 1)
    er[pl.ds(k, 1)] = total[None]
    e_c = []
    for i in x_order:
        e_c.append(send(er.at[k], er.at[k], e_ss.at[i], e_rs.at[i], xpeer(i)))
    for copy in e_c:
        copy.wait_recv()
    whole = er[0]
    for kk in range(1, nf):
        whole = whole + er[kk]
    energy[...] = whole[:, :CHAINS]
    for copy in copies:
        copy.wait_send()


def hand_over(a, b, c, d, a_out, b_out, c_out, d_out):
    a_out[...] = a[...]
    b_out[...] = b[...]
    c_out[...] = c[...]
    d_out[...] = d[...]


def body(observations, labels, tile_live, tile_group, position, momentum, gradient, prior_mean, prior_prec, inv_mass):
    tiles, quarter, row_count = observations.shape
    groups, width = position.shape
    chains = width // quarter
    nf = lax.axis_size("feat")
    half_w = width // 2
    share = tiles // nf
    S = NY * NC
    V = pltpu.VMEM
    D = pltpu.SemaphoreType.DMA
    S = NY * NC
    scratch = [
        V((tiles, row_count), jnp.int32),
        V((1, tiles), jnp.int32),
        V((1, tiles), jnp.int32),
        V((groups, width), F32),
        V((groups, width), F32),
        V((groups, width), F32),
        V((1, width), F32),
        V((1, quarter), F32),
        V((1, quarter), F32),
        D((9,)),
        V((share, nf * quarter, row_count), BF),
        V((width, width), BF),
        V((share, row_count), F32),
        V((tiles, LANES), F32),
        V((groups, width), F32),
        V((tiles, LANES), BF),
        V((2, NY, GRP, half_w), BF),
        V((2, 1, S * 2 * NY), F32),
        V((2, S, 1, S * 2 * NY), F32),
        V((S * 2 * NY, S * 2 * NY), BF),
        V((2, tiles, S * 2 * NY), BF),
        V((2, S * 2 * NY, tiles), BF),
        V((2, S * 2 * NY, LANES), BF),
        V((2, LANES, S * 2 * NY), BF),
        V((2, S, 2 * NY, half_w), BF),
        V((2, S, 2 * NY, half_w), BF),
        V((2, nf, share, half_w), BF),
        V((2, nf, share, half_w), BF),
        V((2, nf, share, half_w), BF),
        V((2, nf, share, half_w), BF),
        V((CHAINS * share, LANES), F32),
        V((CHAINS * share, LANES), F32),
        V((CHAINS * share, LANES), F32),
        V((CHAINS * share, LANES), BF),
        V((2, S, 2 * NY, half_w + LANES), BF),
        V((2, S, 2 * NY, half_w + LANES), BF),
        V((2, NY, GRP, half_w + LANES), BF),
        V((2, NY, GRP, half_w + LANES), BF),
        V((nf, groups, LANES), F32),
        D((nf,)),
        D((nf,)),
        D(()),
        D((2, NY)),
        D((2, NY)),
        D((2, S)),
        D((2, S)),
        D((2, S)),
        D((2, S)),
        D((2, nf)),
        D((2, nf)),
        D((2, nf)),
        D((2, nf)),
        D((2, S)),
        D((2, S)),
        D((2, NY)),
        D((2, NY)),
        D((nf,)),
        D((nf,)),
    ]
    vm = pl.BlockSpec(memory_space=pltpu.VMEM)
    shapes = (
        jax.ShapeDtypeStruct((groups, width), F32),
        jax.ShapeDtypeStruct((groups, width), F32),
        jax.ShapeDtypeStruct((groups, width), F32),
        jax.ShapeDtypeStruct((groups, chains), F32),
    )
    results = pl.pallas_call(
        kernel,
        out_shape=shapes,
        in_specs=[pl.BlockSpec(memory_space=pltpu.HBM)] * 10,
        out_specs=(vm, vm, vm, vm),
        scratch_shapes=scratch,
        compiler_params=pltpu.CompilerParams(collective_id=0, has_side_effects=True),
        name="leapfrog",
    )(
        observations,
        labels,
        tile_live[None, :],
        tile_group[None, :],
        position,
        momentum,
        gradient,
        prior_mean[None, :],
        prior_prec[None, :],
        inv_mass[None, :],
    )
    return pl.pallas_call(
        hand_over,
        out_shape=shapes,
        in_specs=[vm] * 4,
        out_specs=(vm, vm, vm, vm),
        name="hand_over",
    )(*results)


def solution(mesh):
    placed = (
        P("dp", "feat", None),
        P("dp", None),
        P("dp"),
        P("dp"),
        P("dp", "feat"),
        P("dp", "feat"),
        P("dp", "feat"),
        P("feat"),
        P("feat"),
        P("feat"),
    )
    return jax.shard_map(
        body,
        mesh=mesh,
        in_specs=placed,
        out_specs=(P("dp", "feat"), P("dp", "feat"), P("dp", "feat"), P("dp", None)),
        check_vma=False,
    )
```

```python
import functools

import jax
import jax.numpy as jnp
from jax import lax
from jax.experimental import pallas as pl
from jax.experimental.pallas import tpu as pltpu
from jax.sharding import PartitionSpec as P

MESH = pl.DeviceIdType.MESH
step_size = 0.1

NY = 8
NC = 2
CHAINS = 16
HALVES = 1
GRP = 16
LANES = 128
BF = jnp.bfloat16
F32 = jnp.float32


def far_first(n):
    return sorted(range(1, n), key=lambda i: -min(i, n - i))


def dot(a, b, contract=((1,), (0,))):
    return lax.dot_general(a, b, (contract, ((), ())), preferred_element_type=F32)


def one_hot(flags):
    return jnp.where(flags, 1.0, 0.0).astype(BF)


def kernel(
    obs,
    lab_h,
    live_h,
    tg_h,
    pos_h,
    mom_h,
    grd_h,
    pm_h,
    pp_h,
    im_h,
    new_pos,
    new_mom,
    new_grd,
    energy,
    lab,
    live,
    tg,
    pos,
    mom,
    grd,
    pm,
    ppim_p,
    ppim_m,
    in_s,
    obs_v,
    obsx,
    perm,
    labf,
    mask,
    half_s,
    ltile,
    gat,
    rqs,
    rq,
    fold,
    tmat,
    tmat_t,
    smat,
    smat_t,
    sels,
    selr,
    xs,
    xr,
    gs,
    gr,
    wf,
    gf,
    lg,
    res,
    ms,
    mr,
    ls,
    lr,
    zs,
    zr,
    ys,
    yr,
    er,
    obs_ss,
    obs_rs,
    own_s,
    gat_ss,
    gat_rs,
    rq_ss,
    rq_rs,
    sel_ss,
    sel_rs,
    x_ss,
    x_rs,
    gx_ss,
    gx_rs,
    m_ss,
    m_rs,
    l_ss,
    l_rs,
    z_ss,
    z_rs,
    y_ss,
    y_rs,
    e_ss,
    e_rs,
):
    d = lax.axis_index("dp")
    k = lax.axis_index("feat")
    y, z, c = d // (NY * NC), (d // NC) % NY, d % NC
    tiles = lab_h.shape[0]
    nf = 4
    share = tiles // nf
    part_t = share // HALVES
    width = pos_h.shape[1]
    quarter = width // CHAINS
    half_w = width // 2

    def at(yy, zz, cc):
        return ((yy * NY + zz) * NC + cc, k)

    def xpeer(i):
        return (d, (k + i) % nf)

    g_me = (y, z)
    s_me = (z * NC + c, y * NC + c)

    def g_peer(a, i):
        return at((y + i) % NY, z, c) if a == 0 else at(y, (z + i) % NY, c)

    def s_peer(a, i):
        q = (s_me[a] + i) % (NY * NC)
        return at(y, q // NC, q % NC) if a == 0 else at(q // NC, z, q % NC)

    x_order = (2, 1, 3)
    g_order = far_first(NY)
    s_order = far_first(NY * NC)

    barrier = pltpu.get_barrier_semaphore()
    greet = []
    for i in g_order:
        greet += [g_peer(0, i), g_peer(1, i)]
    for i in g_order:
        greet += [at((y + i) % NY, z, 1 - c), at(y, (z + i) % NY, 1 - c)]
    greet += [xpeer(i) for i in x_order] + [at(y, z, 1 - c)]
    for who in greet:
        pl.semaphore_signal(barrier, inc=1, device_id=who, device_id_type=MESH)
    count = len(greet)

    loads = []
    for i, (far, near) in enumerate(
        (
            (tg_h, tg),
            (pp_h, ppim_p),
            (im_h, ppim_m),
            (pos_h, pos),
            (mom_h, mom),
            (grd_h, grd),
            (pm_h, pm),
            (live_h, live),
            (lab_h, lab),
            (obs, obs_v),
        )
    ):
        loads.append(pltpu.make_async_copy(far, near, in_s.at[i]))
        loads[-1].start()

    src = lax.broadcasted_iota(jnp.int32, (LANES, width), 0)
    dst = lax.broadcasted_iota(jnp.int32, (LANES, width), 1)
    want = (dst % quarter) * CHAINS + dst // quarter
    for b in range(width // LANES):
        perm[b * LANES : (b + 1) * LANES, :] = one_hot(src + b * LANES == want)

    for copy in loads[1:7]:
        copy.wait()
    row8 = lax.broadcasted_iota(jnp.int32, (8, quarter), 0)
    pieces = jnp.zeros((8, quarter), F32)
    for n, ref in enumerate((ppim_p, ppim_m)):
        rest = ref[...]
        for m in range(3):
            piece = rest.astype(BF).astype(F32)
            pieces = jnp.where(row8 == 3 * n + m, piece, pieces)
            rest = rest - piece
    feature = lax.broadcasted_iota(jnp.int32, (quarter, width), 0)
    chain_lane = lax.broadcasted_iota(jnp.int32, (quarter, width), 1)
    spread = dot(pieces.astype(BF), one_hot(chain_lane // CHAINS == feature))
    pp = (spread[0:1, :] + spread[1:2, :]) + spread[2:3, :]
    im = (spread[3:4, :] + spread[4:5, :]) + spread[5:6, :]

    half = mom[...] - 0.5 * step_size * grd[...]
    moved = pos[...] + step_size * im * half
    half_s[...] = half
    new_pos[...] = moved
    block = dot(moved.astype(BF), perm[...]).astype(BF)
    for a in range(2):
        gat[a, pl.ds(g_me[a], 1)] = block[None, :, a * half_w : (a + 1) * half_w]

    loads[0].wait()
    tile_row = jnp.broadcast_to(tg[...], (tiles, tiles))
    tile_col = jnp.transpose(tile_row.astype(F32)).astype(jnp.int32)
    own_row, own_col = tile_row // GRP, tile_col // GRP
    t_row = lax.broadcasted_iota(jnp.int32, (tiles, tiles), 1)
    t_col = lax.broadcasted_iota(jnp.int32, (tiles, tiles), 0)
    same = own_row == own_col
    rank_row = jnp.sum(jnp.where(same & (t_col < t_row), 1.0, 0.0), axis=0, keepdims=True)
    rank_row = jnp.broadcast_to(rank_row, (tiles, tiles))
    rank_col = jnp.transpose(rank_row).astype(jnp.int32)
    rank_row = rank_row.astype(jnp.int32)
    slots = NY * NC * NY * 2

    def slot_of(a, own, rank):
        oy, oz, oc = own // (NY * NC), (own // NC) % NY, own % NC
        first, second = (oy, oz) if a == 0 else (oz, oy)
        return (second * NC + oc) * (NY * 2) + first * 2 + rank, first

    for b in range(slots // LANES):
        here = lax.broadcasted_iota(jnp.int32, (LANES, slots), 0) + b * LANES
        there = lax.broadcasted_iota(jnp.int32, (LANES, slots), 1)
        fold[b * LANES : (b + 1) * LANES, :] = one_hot(here % (NY * 2) == there % (NY * 2))
    lane_q = lax.broadcasted_iota(jnp.int32, (NY * NC, slots), 1) // (NY * 2)
    row_q = lax.broadcasted_iota(jnp.int32, (NY * NC, slots), 0)
    for a in range(2):
        s_r, first = slot_of(a, own_row, rank_row)
        asked = (first * GRP + tile_row % GRP + 1)[:16, :].astype(F32).astype(BF)
        s_c, _ = slot_of(a, own_col, rank_col)
        for b in range(slots // LANES):
            tmat[a, :, b * LANES : (b + 1) * LANES] = one_hot(s_c == t_row + b * LANES)
            tmat_t[a, b * LANES : (b + 1) * LANES, :] = one_hot(s_r == t_col + b * LANES)
        wanted = jnp.broadcast_to(dot(asked, tmat[a])[:1, :], (NY * NC, slots))
        spread_q = dot(jnp.where(lane_q == row_q, wanted, 0.0).astype(BF), fold[...])
        placed = jnp.where(lane_q == s_me[a], spread_q, 0.0)
        for q in range(NY * NC):
            rqs[a, q] = placed[q : q + 1, :]

    pl.semaphore_wait(barrier, count)

    copies = []

    def send(src_ref, dst_ref, ss, rs, who):
        copy = pltpu.make_async_remote_copy(
            src_ref=src_ref, dst_ref=dst_ref, send_sem=ss, recv_sem=rs, device_id=who, device_id_type=MESH
        )
        copy.start()
        copies.append(copy)
        return copy

    gat_c = [[], []]
    rq_c = [[], []]
    hops = {}
    for i in s_order:
        hops.setdefault(min(i // NC, NY - i // NC), []).append(i)
    for far in sorted(hops, reverse=True):
        for i in hops[far]:
            for a in range(2):
                q = (s_me[a] + i) % (NY * NC)
                rq_c[a].append(
                    send(rqs.at[a, q], rq.at[a, s_me[a]], rq_ss.at[a, i], rq_rs.at[a, i], s_peer(a, i))
                )
        for i in g_order:
            if min(i, NY - i) == far:
                for a in range(2):
                    ref = gat.at[a, g_me[a]]
                    gat_c[a].append(send(ref, ref, gat_ss.at[a, i], gat_rs.at[a, i], g_peer(a, i)))
    loads[9].wait()
    obs_c = []
    for i in x_order:
        to = (k + i) % nf
        obs_c.append(
            send(
                obs_v.at[pl.ds(to * share, share)],
                obsx.at[:, pl.ds(pl.multiple_of(k * quarter, quarter), quarter), :],
                obs_ss.at[i],
                obs_rs.at[i],
                xpeer(i),
            )
        )
    own_copy = pltpu.make_async_copy(
        obs.at[pl.ds(k * share, share)],
        obsx.at[:, pl.ds(pl.multiple_of(k * quarter, quarter), quarter), :],
        own_s,
    )
    own_copy.start()

    loads[7].wait()
    loads[8].wait()
    rows = pl.ds(pl.multiple_of(k * share, share), share)
    labf[...] = lab[rows, :].astype(F32)
    live_col = jnp.transpose(jnp.broadcast_to(live[...], (tiles, tiles)).astype(F32))
    mask[...] = jnp.where(t_row.astype(F32) < live_col, 1.0, 0.0)
    ltile[...] = jnp.zeros_like(ltile)
    for a in range(2):
        rq[a, pl.ds(s_me[a], 1)] = rqs[a, pl.ds(s_me[a], 1)]
        for copy in rq_c[a]:
            copy.wait_recv()
    for a in range(2):
        ask = jnp.sum(rq[a].reshape(NY * NC, slots), axis=0, keepdims=True)
        for b in range(slots // LANES):
            part = jnp.broadcast_to(ask[:, b * LANES : (b + 1) * LANES], (LANES, LANES))
            chosen = jnp.where(part == (t_col + 1).astype(F32), 1.0, 0.0)
            smat_t[a, :, b * LANES : (b + 1) * LANES] = chosen.astype(BF)
            smat[a, b * LANES : (b + 1) * LANES, :] = jnp.transpose(chosen).astype(BF)
    for a in range(2):
        for copy in gat_c[a]:
            copy.wait_recv()
    for a in range(2):
        table = gat[a].reshape(NY * GRP, half_w)
        sels[a] = dot(smat[a], table).astype(BF).reshape(NY * NC, NY * 2, half_w)
    sel_c = []
    for i in s_order:
        for a in range(2):
            q = (s_me[a] + i) % (NY * NC)
            sel_c.append(send(sels.at[a, q], selr.at[a, s_me[a]], sel_ss.at[a, i], sel_rs.at[a, i], s_peer(a, i)))
    for a in range(2):
        selr[a, pl.ds(s_me[a], 1)] = sels[a, pl.ds(s_me[a], 1)]

    for copy in sel_c:
        copy.wait_recv()
    for a in range(2):
        rows_a = dot(tmat[a], selr[a].reshape(slots, half_w)).astype(BF)
        xs[a] = rows_a.reshape(nf, HALVES, part_t, half_w)
    x_c = []
    for h in range(HALVES):
        for i in x_order:
            for a in range(2):
                to = (k + i) % nf
                x_c.append(
                    (h, send(xs.at[a, to, h], xr.at[a, h, k], x_ss.at[a, h, i], x_rs.at[a, h, i], xpeer(i)))
                )
        for a in range(2):
            xr[a, h, pl.ds(k, 1)] = xs[a, pl.ds(k, 1), h]

    lane = lax.broadcasted_iota(jnp.int32, (part_t, LANES), 1) // quarter
    per = LANES // quarter
    lane16 = lax.broadcasted_iota(jnp.int32, (CHAINS, LANES), 1)
    loglik = jnp.zeros((CHAINS, LANES), F32)
    gx_c = []
    for h in range(HALVES):
        for hh, copy in x_c:
            if hh == h:
                copy.wait_recv()
        for a in range(2):
            for b in range(half_w // LANES):
                came = [xr[a, h, kk, :, b * LANES : (b + 1) * LANES].astype(F32) for kk in range(nf)]
                for ci in range(per):
                    out = jnp.zeros((part_t, LANES), F32)
                    for kk in range(nf):
                        shift = ((kk - ci) * quarter) % LANES
                        moved_k = came[kk] if shift == 0 else pltpu.roll(came[kk], shift, 1)
                        out = jnp.where(lane == kk, moved_k, out)
                    chain = a * (CHAINS // 2) + b * per + ci
                    wf[h, chain * part_t : (chain + 1) * part_t, :] = out
        if h == 0:
            own_copy.wait()
            for copy in obs_c:
                copy.wait_recv()
        for n in range(part_t):
            coeff = wf[h, pl.ds(n, CHAINS, stride=part_t), :].astype(BF)
            lg[h, n * CHAINS : (n + 1) * CHAINS, :] = dot(coeff, obsx[h * part_t + n])
        for n in range(part_t):
            t = h * part_t + n
            logits = lg[h, n * CHAINS : (n + 1) * CHAINS, :]
            target = jnp.broadcast_to(labf[t : t + 1, :], (CHAINS, LANES))
            alive = jnp.broadcast_to(mask[pl.ds(k * share + t, 1), :], (CHAINS, LANES)) > 0.5
            e = jnp.exp(-jnp.abs(logits))
            r = 1.0 / (1.0 + e)
            sig = jnp.where(logits >= 0.0, r, e * r)
            res[h, n * CHAINS : (n + 1) * CHAINS, :] = jnp.where(alive, sig - target, 0.0).astype(BF)
            soft = jnp.maximum(logits, 0.0) + jnp.log1p(e)
            term = jnp.where(alive, soft - target * logits, 0.0)
            loglik = jnp.where(lane16 == t, jnp.sum(term, axis=1, keepdims=True), loglik)
        for n in range(part_t):
            back = dot(res[h, n * CHAINS : (n + 1) * CHAINS, :], obsx[h * part_t + n], ((1,), (1,)))
            gf[h, pl.ds(n, CHAINS, stride=part_t), :] = back
        for a in range(2):
            for b in range(half_w // LANES):
                chain = a * (CHAINS // 2) + b * per
                made = [gf[h, (chain + ci) * part_t : (chain + ci + 1) * part_t, :] for ci in range(per)]
                for kk in range(nf):
                    out = jnp.zeros((part_t, LANES), F32)
                    for ci in range(per):
                        shift = ((ci - kk) * quarter) % LANES
                        moved_c = made[ci] if shift == 0 else pltpu.roll(made[ci], shift, 1)
                        out = jnp.where(lane == ci, moved_c, out)
                    gs[a, h, kk, :, b * LANES : (b + 1) * LANES] = out.astype(BF)
        for i in x_order:
            for a in range(2):
                to = (k + i) % nf
                gx_c.append(send(gs.at[a, h, to], gr.at[a, k, h], gx_ss.at[a, h, i], gx_rs.at[a, h, i], xpeer(i)))
        for a in range(2):
            gr[a, pl.ds(k, 1), h] = gs[a, h, pl.ds(k, 1)]

    high = loglik.astype(BF).astype(F32)
    both = jnp.concatenate([high, loglik - high, jnp.zeros((LANES - 2 * CHAINS, LANES), F32)], axis=0)
    ltile[rows, :] = jnp.transpose(both)[:share, :].astype(BF)
    ls[...] = dot(tmat_t[0], ltile[...]).astype(BF).reshape(NY * NC, NY * 2, LANES)
    l_c = []
    for i in s_order:
        q = (s_me[0] + i) % (NY * NC)
        l_c.append(send(ls.at[q], lr.at[s_me[0]], l_ss.at[i], l_rs.at[i], s_peer(0, i)))
    lr[pl.ds(s_me[0], 1)] = ls[pl.ds(s_me[0], 1)]

    for copy in gx_c:
        copy.wait_recv()
    for a in range(2):
        sent = dot(tmat_t[a], gr[a].reshape(tiles, half_w)).astype(BF)
        ms[a] = sent.reshape(NY * NC, NY * 2, half_w)
    m_c = []
    for i in s_order:
        for a in range(2):
            q = (s_me[a] + i) % (NY * NC)
            m_c.append(send(ms.at[a, q], mr.at[a, s_me[a]], m_ss.at[a, i], m_rs.at[a, i], s_peer(a, i)))
    for a in range(2):
        mr[a, pl.ds(s_me[a], 1)] = ms[a, pl.ds(s_me[a], 1)]

    for copy in l_c:
        copy.wait_recv()
    zs[...] = dot(smat_t[0], lr[...].reshape(slots, LANES)).astype(BF).reshape(NY, GRP, LANES)
    z_c = []
    for i in g_order:
        to = (g_me[0] + i) % NY
        z_c.append(send(zs.at[to], zr.at[g_me[0]], z_ss.at[i], z_rs.at[i], g_peer(0, i)))
    zr[pl.ds(g_me[0], 1)] = zs[pl.ds(g_me[0], 1)]

    offset = new_pos[...] - pm[...]
    prior_term = pp * offset
    prior_quad = prior_term * offset

    for copy in m_c:
        copy.wait_recv()
    for a in range(2):
        summed = dot(smat_t[a], mr[a].reshape(slots, half_w)).astype(BF)
        ys[a] = summed.reshape(NY, GRP, half_w)
    y_c = []
    for i in g_order:
        for a in range(2):
            to = (g_me[a] + i) % NY
            y_c.append(send(ys.at[a, to], yr.at[a, g_me[a]], y_ss.at[a, i], y_rs.at[a, i], g_peer(a, i)))
    for a in range(2):
        yr[a, pl.ds(g_me[a], 1)] = ys[a, pl.ds(g_me[a], 1)]

    lik = jnp.zeros((GRP, width), F32)
    group_loglik = jnp.zeros((GRP, LANES), F32)
    for copy in z_c:
        copy.wait_recv()
    for g in range(NY):
        group_loglik = group_loglik + zr[g].astype(F32)
    group_loglik = group_loglik + pltpu.roll(group_loglik, LANES - CHAINS, 1)
    for copy in y_c:
        copy.wait_recv()
    for a in range(2):
        part = yr[a].reshape(NY * GRP, half_w)
        back = dot(part, perm[:, a * half_w : (a + 1) * half_w], ((1,), (1,)))
        for g in range(NY):
            lik = lik + back[g * GRP : (g + 1) * GRP, :]

    grad_now = lik + prior_term
    mom_now = half_s[...] - 0.5 * step_size * grad_now
    new_grd[...] = grad_now
    new_mom[...] = mom_now
    quad = 0.5 * (prior_quad + im * mom_now * mom_now)
    total = quad[:, :LANES]
    for b in range(1, width // LANES):
        total = total + quad[:, b * LANES : (b + 1) * LANES]
    shift = LANES // 2
    while shift >= CHAINS:
        total = total + pltpu.roll(total, shift, 1)
        shift //= 2
    total = total + group_loglik
    er[pl.ds(k, 1)] = total[None]
    e_c = []
    for i in x_order:
        e_c.append(send(er.at[k], er.at[k], e_ss.at[i], e_rs.at[i], xpeer(i)))
    for copy in copies[: -len(e_c)]:
        copy.wait_send()
    for copy in e_c:
        copy.wait_recv()
    whole = er[0]
    for kk in range(1, nf):
        whole = whole + er[kk]
    energy[...] = whole[:, :CHAINS]
    for copy in e_c:
        copy.wait_send()


def hand_over(a, b, c, d, a_out, b_out, c_out, d_out):
    a_out[...] = a[...]
    b_out[...] = b[...]
    c_out[...] = c[...]
    d_out[...] = d[...]


def body(observations, labels, tile_live, tile_group, position, momentum, gradient, prior_mean, prior_prec, inv_mass):
    tiles, quarter, row_count = observations.shape
    groups, width = position.shape
    chains = width // quarter
    nf = lax.axis_size("feat")
    half_w = width // 2
    share = tiles // nf
    S = NY * NC
    part_t = share // HALVES
    V = pltpu.VMEM
    D = pltpu.SemaphoreType.DMA
    S = NY * NC
    scratch = [
        V((tiles, row_count), jnp.int32),
        V((1, tiles), jnp.int32),
        V((1, tiles), jnp.int32),
        V((groups, width), F32),
        V((groups, width), F32),
        V((groups, width), F32),
        V((1, width), F32),
        V((1, quarter), F32),
        V((1, quarter), F32),
        D((10,)),
        V((tiles, quarter, row_count), BF),
        V((share, nf * quarter, row_count), BF),
        V((width, width), BF),
        V((share, row_count), F32),
        V((tiles, LANES), F32),
        V((groups, width), F32),
        V((tiles, LANES), BF),
        V((2, NY, GRP, half_w), BF),
        V((2, S, 1, S * 2 * NY), F32),
        V((2, S, 1, S * 2 * NY), F32),
        V((S * 2 * NY, S * 2 * NY), BF),
        V((2, tiles, S * 2 * NY), BF),
        V((2, S * 2 * NY, tiles), BF),
        V((2, S * 2 * NY, LANES), BF),
        V((2, LANES, S * 2 * NY), BF),
        V((2, S, 2 * NY, half_w), BF),
        V((2, S, 2 * NY, half_w), BF),
        V((2, nf, HALVES, part_t, half_w), BF),
        V((2, HALVES, nf, part_t, half_w), BF),
        V((2, HALVES, nf, part_t, half_w), BF),
        V((2, nf, HALVES, part_t, half_w), BF),
        V((HALVES, CHAINS * part_t, LANES), F32),
        V((HALVES, CHAINS * part_t, LANES), F32),
        V((HALVES, CHAINS * part_t, LANES), F32),
        V((HALVES, CHAINS * part_t, LANES), BF),
        V((2, S, 2 * NY, half_w), BF),
        V((2, S, 2 * NY, half_w), BF),
        V((S, 2 * NY, LANES), BF),
        V((S, 2 * NY, LANES), BF),
        V((NY, GRP, LANES), BF),
        V((NY, GRP, LANES), BF),
        V((2, NY, GRP, half_w), BF),
        V((2, NY, GRP, half_w), BF),
        V((nf, groups, LANES), F32),
        D((nf,)),
        D((nf,)),
        D(()),
        D((2, NY)),
        D((2, NY)),
        D((2, S)),
        D((2, S)),
        D((2, S)),
        D((2, S)),
        D((2, HALVES, nf)),
        D((2, HALVES, nf)),
        D((2, HALVES, nf)),
        D((2, HALVES, nf)),
        D((2, S)),
        D((2, S)),
        D((S,)),
        D((S,)),
        D((NY,)),
        D((NY,)),
        D((2, NY)),
        D((2, NY)),
        D((nf,)),
        D((nf,)),
    ]
    vm = pl.BlockSpec(memory_space=pltpu.VMEM)
    shapes = (
        jax.ShapeDtypeStruct((groups, width), F32),
        jax.ShapeDtypeStruct((groups, width), F32),
        jax.ShapeDtypeStruct((groups, width), F32),
        jax.ShapeDtypeStruct((groups, chains), F32),
    )
    results = pl.pallas_call(
        kernel,
        out_shape=tuple(pltpu.VMEM(x.shape, x.dtype) for x in shapes),
        in_specs=[pl.BlockSpec(memory_space=pltpu.HBM)] * 10,
        out_specs=(vm, vm, vm, vm),
        scratch_shapes=scratch,
        compiler_params=pltpu.CompilerParams(collective_id=0, has_side_effects=True),
        name="leapfrog",
    )(
        observations,
        labels,
        tile_live[None, :],
        tile_group[None, :],
        position,
        momentum,
        gradient,
        prior_mean[None, :],
        prior_prec[None, :],
        inv_mass[None, :],
    )
    return pl.pallas_call(
        hand_over,
        out_shape=shapes,
        in_specs=[vm] * 4,
        out_specs=(vm, vm, vm, vm),
        name="hand_over",
    )(*(pltpu.with_memory_space_constraint(x, pltpu.VMEM) for x in results))


def solution(mesh):
    placed = (
        P("dp", "feat", None),
        P("dp", None),
        P("dp"),
        P("dp"),
        P("dp", "feat"),
        P("dp", "feat"),
        P("dp", "feat"),
        P("feat"),
        P("feat"),
        P("feat"),
    )
    return jax.shard_map(
        body,
        mesh=mesh,
        in_specs=placed,
        out_specs=(P("dp", "feat"), P("dp", "feat"), P("dp", "feat"), P("dp", None)),
        check_vma=False,
    )
```

```python
import functools

import jax
import jax.numpy as jnp
from jax import lax
from jax.experimental import pallas as pl
from jax.experimental.pallas import tpu as pltpu
from jax.sharding import PartitionSpec as P

MESH = pl.DeviceIdType.MESH
step_size = 0.1

NY = 8
NC = 2
CHAINS = 16
HALVES = 2
GRP = 16
LANES = 128
BF = jnp.bfloat16
F32 = jnp.float32


def far_first(n):
    return sorted(range(1, n), key=lambda i: -min(i, n - i))


def dot(a, b, contract=((1,), (0,))):
    return lax.dot_general(a, b, (contract, ((), ())), preferred_element_type=F32)


def one_hot(flags):
    return jnp.where(flags, 1.0, 0.0).astype(BF)


def kernel(
    obs,
    lab_h,
    live_h,
    tg_h,
    pos_h,
    mom_h,
    grd_h,
    pm_h,
    pp_h,
    im_h,
    new_pos,
    new_mom,
    new_grd,
    energy,
    lab,
    live,
    tg,
    pos,
    mom,
    grd,
    pm,
    ppim_p,
    ppim_m,
    in_s,
    obs_v,
    obsx,
    perm,
    labf,
    mask,
    half_s,
    ltile,
    lab_r,
    live_r,
    lt_s,
    lt_r,
    gat,
    rqs,
    rq,
    fold,
    tmat,
    tmat_t,
    smat,
    smat_t,
    sels,
    selr,
    xs,
    xr,
    gs,
    gr,
    wf,
    gf,
    lg,
    res,
    ms,
    mr,
    ls,
    lr,
    zs,
    zr,
    ys,
    yr,
    er,
    obs_ss,
    obs_rs,
    lab_ss,
    lab_rs,
    gat_ss,
    gat_rs,
    rq_ss,
    rq_rs,
    sel_ss,
    sel_rs,
    x_ss,
    x_rs,
    gx_ss,
    gx_rs,
    m_ss,
    m_rs,
    l_ss,
    l_rs,
    z_ss,
    z_rs,
    y_ss,
    y_rs,
    e_ss,
    e_rs,
):
    d = lax.axis_index("dp")
    k = lax.axis_index("feat")
    y, z, c = d // (NY * NC), (d // NC) % NY, d % NC
    tiles = lab_h.shape[0]
    nf = 4
    share = tiles // nf
    part_t = share // HALVES
    width = pos_h.shape[1]
    quarter = width // CHAINS
    half_w = width // 2

    def at(yy, zz, cc):
        return ((yy * NY + zz) * NC + cc, k)

    def xpeer(i):
        return (d, (k + i) % nf)

    def xcross(i):
        return (d + 1 - 2 * c, (k + i) % nf)

    g_me = (y, z)
    s_me = (z * NC + c, y * NC + c)

    def g_peer(a, i):
        return at((y + i) % NY, z, c) if a == 0 else at(y, (z + i) % NY, c)

    def s_peer(a, i):
        q = (s_me[a] + i) % (NY * NC)
        return at(y, q // NC, q % NC) if a == 0 else at(q // NC, z, q % NC)

    x_order = (2, 1, 3)
    g_order = far_first(NY)
    x_all = x_order + (0,)
    s_order = far_first(NY * NC)

    barrier = pltpu.get_barrier_semaphore()
    greet = []
    for i in g_order:
        for cc in (c, 1 - c):
            greet += [at((y + i) % NY, z, cc), at(y, (z + i) % NY, cc)]
    greet += [xpeer(i) for i in x_order] + [xcross(i) for i in x_all]
    for who in greet:
        pl.semaphore_signal(barrier, inc=1, device_id=who, device_id_type=MESH)
    count = len(greet)

    loads = []
    for i, (far, near) in enumerate(
        (
            (tg_h, tg),
            (pp_h, ppim_p),
            (im_h, ppim_m),
            (pos_h, pos),
            (mom_h, mom),
            (grd_h, grd),
            (pm_h, pm),
            (live_h, live),
            (lab_h, lab),
            (obs, obs_v),
        )
    ):
        loads.append(pltpu.make_async_copy(far, near, in_s.at[i]))
        loads[-1].start()

    src = lax.broadcasted_iota(jnp.int32, (LANES, width), 0)
    dst = lax.broadcasted_iota(jnp.int32, (LANES, width), 1)
    want = (dst % quarter) * CHAINS + dst // quarter
    for b in range(width // LANES):
        perm[b * LANES : (b + 1) * LANES, :] = one_hot(src + b * LANES == want)

    for copy in loads[1:7]:
        copy.wait()
    row8 = lax.broadcasted_iota(jnp.int32, (8, quarter), 0)
    pieces = jnp.zeros((8, quarter), F32)
    for n, ref in enumerate((ppim_p, ppim_m)):
        rest = ref[...]
        for m in range(3):
            piece = rest.astype(BF).astype(F32)
            pieces = jnp.where(row8 == 3 * n + m, piece, pieces)
            rest = rest - piece
    feature = lax.broadcasted_iota(jnp.int32, (quarter, width), 0)
    chain_lane = lax.broadcasted_iota(jnp.int32, (quarter, width), 1)
    spread = dot(pieces.astype(BF), one_hot(chain_lane // CHAINS == feature))
    pp = (spread[0:1, :] + spread[1:2, :]) + spread[2:3, :]
    im = (spread[3:4, :] + spread[4:5, :]) + spread[5:6, :]

    half = mom[...] - 0.5 * step_size * grd[...]
    moved = pos[...] + step_size * im * half
    half_s[...] = half
    new_pos[...] = moved
    block = dot(moved.astype(BF), perm[...]).astype(BF)
    for a in range(2):
        gat[a, pl.ds(g_me[a], 1)] = block[None, :, a * half_w : (a + 1) * half_w]

    loads[0].wait()
    tile_row = jnp.broadcast_to(tg[...], (tiles, tiles))
    tile_col = jnp.transpose(tile_row.astype(F32)).astype(jnp.int32)
    own_row, own_col = tile_row // GRP, tile_col // GRP
    t_row = lax.broadcasted_iota(jnp.int32, (tiles, tiles), 1)
    t_col = lax.broadcasted_iota(jnp.int32, (tiles, tiles), 0)
    same = own_row == own_col
    rank_row = jnp.sum(jnp.where(same & (t_col < t_row), 1.0, 0.0), axis=0, keepdims=True)
    rank_row = jnp.broadcast_to(rank_row, (tiles, tiles))
    rank_col = jnp.transpose(rank_row).astype(jnp.int32)
    rank_row = rank_row.astype(jnp.int32)
    slots = NY * NC * NY * 2

    def slot_of(a, own, rank):
        oy, oz, oc = own // (NY * NC), (own // NC) % NY, own % NC
        first, second = (oy, oz) if a == 0 else (oz, oy)
        return (second * NC + oc) * (NY * 2) + first * 2 + rank, first

    for b in range(slots // LANES):
        here = lax.broadcasted_iota(jnp.int32, (LANES, slots), 0) + b * LANES
        there = lax.broadcasted_iota(jnp.int32, (LANES, slots), 1)
        fold[b * LANES : (b + 1) * LANES, :] = one_hot(here % (NY * 2) == there % (NY * 2))
    lane_q = lax.broadcasted_iota(jnp.int32, (NY * NC, slots), 1) // (NY * 2)
    row_q = lax.broadcasted_iota(jnp.int32, (NY * NC, slots), 0)
    for a in range(2):
        s_r, first = slot_of(a, own_row, rank_row)
        asked = (first * GRP + tile_row % GRP + 1)[:16, :].astype(F32).astype(BF)
        s_c, _ = slot_of(a, own_col, rank_col)
        for b in range(slots // LANES):
            tmat[a, :, b * LANES : (b + 1) * LANES] = one_hot(s_c == t_row + b * LANES)
            tmat_t[a, b * LANES : (b + 1) * LANES, :] = one_hot(s_r == t_col + b * LANES)
        wanted = jnp.broadcast_to(dot(asked, tmat[a])[:1, :], (NY * NC, slots))
        spread_q = dot(jnp.where(lane_q == row_q, wanted, 0.0).astype(BF), fold[...])
        placed = jnp.where(lane_q == s_me[a], spread_q, 0.0)
        for q in range(NY * NC):
            rqs[a, q] = placed[q : q + 1, :]

    pl.semaphore_wait(barrier, count)

    def send(src_ref, dst_ref, ss, rs, who):
        copy = pltpu.make_async_remote_copy(
            src_ref=src_ref, dst_ref=dst_ref, send_sem=ss, recv_sem=rs, device_id=who, device_id_type=MESH
        )
        copy.start()

    def arrived(view, sem):
        pltpu.make_async_copy(view, view, sem).wait()

    for copy in loads[7:]:
        copy.wait()
    mine = pl.ds(pl.multiple_of(k * quarter, quarter), quarter)
    rows = pl.ds(pl.multiple_of(k * share, share), share)
    for i in x_all:
        to = (k + i) % nf
        send(obs_v.at[pl.ds(to * share, share)], obsx.at[:, mine, :], obs_ss, obs_rs, xcross(i))
    send(lab.at[rows], lab_r, lab_ss.at[0], lab_rs.at[0], xcross(0))
    send(live, live_r, lab_ss.at[1], lab_rs.at[1], xcross(0))
    hops = {}
    for i in s_order:
        hops.setdefault(min(i // NC, NY - i // NC), []).append(i)
    for far in sorted(hops, reverse=True):
        for i in hops[far]:
            for a in range(2):
                q = (s_me[a] + i) % (NY * NC)
                send(rqs.at[a, q], rq.at[a, s_me[a]], rq_ss, rq_rs, s_peer(a, i))
        for i in g_order:
            if min(i, NY - i) == far:
                for a in range(2):
                    ref = gat.at[a, g_me[a]]
                    send(ref, ref, gat_ss, gat_rs, g_peer(a, i))
    for a in range(2):
        rq[a, pl.ds(s_me[a], 1)] = rqs[a, pl.ds(s_me[a], 1)]
    arrived(rq.at[:, pl.ds(0, NY * NC - 1)], rq_rs)
    for a in range(2):
        ask = jnp.sum(rq[a].reshape(NY * NC, slots), axis=0, keepdims=True)
        for b in range(slots // LANES):
            part = jnp.broadcast_to(ask[:, b * LANES : (b + 1) * LANES], (LANES, LANES))
            chosen = jnp.where(part == (t_col + 1).astype(F32), 1.0, 0.0)
            smat_t[a, :, b * LANES : (b + 1) * LANES] = chosen.astype(BF)
            smat[a, b * LANES : (b + 1) * LANES, :] = jnp.transpose(chosen).astype(BF)
    arrived(gat.at[:, pl.ds(0, NY - 1)], gat_rs)
    for a in range(2):
        table = gat[a].reshape(NY * GRP, half_w)
        sels[a] = dot(smat[a], table).astype(BF).reshape(NY * NC, NY * 2, half_w)
    for i in s_order:
        for a in range(2):
            q = (s_me[a] + i) % (NY * NC)
            send(sels.at[a, q], selr.at[a, s_me[a]], sel_ss, sel_rs, s_peer(a, i))
    for a in range(2):
        selr[a, pl.ds(s_me[a], 1)] = sels[a, pl.ds(s_me[a], 1)]

    arrived(lab_r, lab_rs.at[0])
    arrived(live_r, lab_rs.at[1])
    labf[...] = lab_r[...].astype(F32)
    live_col = jnp.transpose(jnp.broadcast_to(live_r[...], (tiles, tiles)).astype(F32))
    mask[...] = jnp.where(t_row.astype(F32) < live_col, 1.0, 0.0)
    ltile[...] = jnp.zeros_like(ltile)

    arrived(selr.at[:, pl.ds(0, NY * NC - 1)], sel_rs)
    for a in range(2):
        rows_a = dot(tmat[a], selr[a].reshape(slots, half_w)).astype(BF)
        xs[a] = rows_a.reshape(nf, HALVES, part_t, half_w)
    for h in range(HALVES):
        for i in x_all:
            for a in range(2):
                to = (k + i) % nf
                send(xs.at[a, to, h], xr.at[a, h, k], x_ss, x_rs.at[h], xcross(i))

    lane = lax.broadcasted_iota(jnp.int32, (part_t, LANES), 1) // quarter
    per = LANES // quarter
    lane16 = lax.broadcasted_iota(jnp.int32, (CHAINS, LANES), 1)
    loglik = jnp.zeros((CHAINS, LANES), F32)
    for h in range(HALVES):
        arrived(xr.at[:, h], x_rs.at[h])
        for a in range(2):
            for b in range(half_w // LANES):
                came = [xr[a, h, kk, :, b * LANES : (b + 1) * LANES].astype(F32) for kk in range(nf)]
                for ci in range(per):
                    out = jnp.zeros((part_t, LANES), F32)
                    for kk in range(nf):
                        shift = ((kk - ci) * quarter) % LANES
                        moved_k = came[kk] if shift == 0 else pltpu.roll(came[kk], shift, 1)
                        out = jnp.where(lane == kk, moved_k, out)
                    chain = a * (CHAINS // 2) + b * per + ci
                    wf[h, chain * part_t : (chain + 1) * part_t, :] = out
        if h == 0:
            arrived(obsx, obs_rs)
        for n in range(part_t):
            coeff = wf[h, pl.ds(n, CHAINS, stride=part_t), :].astype(BF)
            lg[h, n * CHAINS : (n + 1) * CHAINS, :] = dot(coeff, obsx[h * part_t + n])
        for n in range(part_t):
            t = h * part_t + n
            logits = lg[h, n * CHAINS : (n + 1) * CHAINS, :]
            target = jnp.broadcast_to(labf[t : t + 1, :], (CHAINS, LANES))
            alive = jnp.broadcast_to(mask[pl.ds(k * share + t, 1), :], (CHAINS, LANES)) > 0.5
            e = jnp.exp(-jnp.abs(logits))
            r = 1.0 / (1.0 + e)
            sig = jnp.where(logits >= 0.0, r, e * r)
            res[h, n * CHAINS : (n + 1) * CHAINS, :] = jnp.where(alive, sig - target, 0.0).astype(BF)
            soft = jnp.maximum(logits, 0.0) + jnp.log1p(e)
            term = jnp.where(alive, soft - target * logits, 0.0)
            loglik = jnp.where(lane16 == t, jnp.sum(term, axis=1, keepdims=True), loglik)
        for n in range(part_t):
            back = dot(res[h, n * CHAINS : (n + 1) * CHAINS, :], obsx[h * part_t + n], ((1,), (1,)))
            gf[h, pl.ds(n, CHAINS, stride=part_t), :] = back
        for a in range(2):
            for b in range(half_w // LANES):
                chain = a * (CHAINS // 2) + b * per
                made = [gf[h, (chain + ci) * part_t : (chain + ci + 1) * part_t, :] for ci in range(per)]
                for kk in range(nf):
                    out = jnp.zeros((part_t, LANES), F32)
                    for ci in range(per):
                        shift = ((ci - kk) * quarter) % LANES
                        moved_c = made[ci] if shift == 0 else pltpu.roll(made[ci], shift, 1)
                        out = jnp.where(lane == ci, moved_c, out)
                    gs[a, h, kk, :, b * LANES : (b + 1) * LANES] = out.astype(BF)
        for i in x_all:
            for a in range(2):
                to = (k + i) % nf
                send(gs.at[a, h, to], gr.at[a, k, h], gx_ss, gx_rs, xcross(i))

    high = loglik.astype(BF).astype(F32)
    both = jnp.concatenate([high, loglik - high, jnp.zeros((LANES - 2 * CHAINS, LANES), F32)], axis=0)
    lt_s[...] = jnp.transpose(both)[:share, :].astype(BF)
    send(lt_s, lt_r, lab_ss.at[2], lab_rs.at[2], xcross(0))
    arrived(lt_r, lab_rs.at[2])
    ltile[rows, :] = lt_r[...]
    ls[...] = dot(tmat_t[0], ltile[...]).astype(BF).reshape(NY * NC, NY * 2, LANES)
    for i in s_order:
        q = (s_me[0] + i) % (NY * NC)
        send(ls.at[q], lr.at[s_me[0]], l_ss, l_rs, s_peer(0, i))
    lr[pl.ds(s_me[0], 1)] = ls[pl.ds(s_me[0], 1)]

    arrived(gr, gx_rs)
    for a in range(2):
        sent = dot(tmat_t[a], gr[a].reshape(tiles, half_w)).astype(BF)
        ms[a] = sent.reshape(NY * NC, NY * 2, half_w)
    for i in s_order:
        for a in range(2):
            q = (s_me[a] + i) % (NY * NC)
            send(ms.at[a, q], mr.at[a, s_me[a]], m_ss, m_rs, s_peer(a, i))
    for a in range(2):
        mr[a, pl.ds(s_me[a], 1)] = ms[a, pl.ds(s_me[a], 1)]

    arrived(lr.at[pl.ds(0, NY * NC - 1)], l_rs)
    zs[...] = dot(smat_t[0], lr[...].reshape(slots, LANES)).astype(BF).reshape(NY, GRP, LANES)
    for i in g_order:
        to = (g_me[0] + i) % NY
        send(zs.at[to], zr.at[g_me[0]], z_ss, z_rs, g_peer(0, i))
    zr[pl.ds(g_me[0], 1)] = zs[pl.ds(g_me[0], 1)]

    offset = new_pos[...] - pm[...]
    prior_term = pp * offset
    prior_quad = prior_term * offset

    arrived(mr.at[:, pl.ds(0, NY * NC - 1)], m_rs)
    for a in range(2):
        summed = dot(smat_t[a], mr[a].reshape(slots, half_w)).astype(BF)
        ys[a] = summed.reshape(NY, GRP, half_w)
    for i in g_order:
        for a in range(2):
            to = (g_me[a] + i) % NY
            send(ys.at[a, to], yr.at[a, g_me[a]], y_ss, y_rs, g_peer(a, i))
    for a in range(2):
        yr[a, pl.ds(g_me[a], 1)] = ys[a, pl.ds(g_me[a], 1)]

    lik = jnp.zeros((GRP, width), F32)
    group_loglik = jnp.zeros((GRP, LANES), F32)
    arrived(zr.at[pl.ds(0, NY - 1)], z_rs)
    for g in range(NY):
        group_loglik = group_loglik + zr[g].astype(F32)
    group_loglik = group_loglik + pltpu.roll(group_loglik, LANES - CHAINS, 1)
    arrived(yr.at[:, pl.ds(0, NY - 1)], y_rs)
    for a in range(2):
        part = yr[a].reshape(NY * GRP, half_w)
        back = dot(part, perm[:, a * half_w : (a + 1) * half_w], ((1,), (1,)))
        for g in range(NY):
            lik = lik + back[g * GRP : (g + 1) * GRP, :]

    grad_now = lik + prior_term
    mom_now = half_s[...] - 0.5 * step_size * grad_now
    new_grd[...] = grad_now
    new_mom[...] = mom_now
    quad = 0.5 * (prior_quad + im * mom_now * mom_now)
    total = quad[:, :LANES]
    for b in range(1, width // LANES):
        total = total + quad[:, b * LANES : (b + 1) * LANES]
    shift = LANES // 2
    while shift >= CHAINS:
        total = total + pltpu.roll(total, shift, 1)
        shift //= 2
    total = total + group_loglik
    er[pl.ds(k, 1)] = total[None]
    for i in x_order:
        send(er.at[k], er.at[k], e_ss, e_rs, xpeer(i))
    for view, sem in (
        (obs_v, obs_ss),
        (rq.at[:, pl.ds(0, NY * NC - 1)], rq_ss),
        (gat.at[:, pl.ds(0, NY - 1)], gat_ss),
        (sels.at[:, pl.ds(0, NY * NC - 1)], sel_ss),
        (xs, x_ss),
        (gs, gx_ss),
        (ls.at[pl.ds(0, NY * NC - 1)], l_ss),
        (ms.at[:, pl.ds(0, NY * NC - 1)], m_ss),
        (zs.at[pl.ds(0, NY - 1)], z_ss),
        (ys.at[:, pl.ds(0, NY - 1)], y_ss),
        (lab_r, lab_ss.at[0]),
        (live_r, lab_ss.at[1]),
        (lt_s, lab_ss.at[2]),
    ):
        arrived(view, sem)
    arrived(er.at[pl.ds(0, nf - 1)], e_rs)
    whole = er[0]
    for kk in range(1, nf):
        whole = whole + er[kk]
    energy[...] = whole[:, :CHAINS]
    arrived(er.at[pl.ds(0, nf - 1)], e_ss)


def hand_over(a, b, c, d, a_out, b_out, c_out, d_out):
    a_out[...] = a[...]
    b_out[...] = b[...]
    c_out[...] = c[...]
    d_out[...] = d[...]


def body(observations, labels, tile_live, tile_group, position, momentum, gradient, prior_mean, prior_prec, inv_mass):
    tiles, quarter, row_count = observations.shape
    groups, width = position.shape
    chains = width // quarter
    nf = lax.axis_size("feat")
    half_w = width // 2
    share = tiles // nf
    S = NY * NC
    part_t = share // HALVES
    V = pltpu.VMEM
    D = pltpu.SemaphoreType.DMA
    S = NY * NC
    scratch = [
        V((tiles, row_count), jnp.int32),
        V((1, tiles), jnp.int32),
        V((1, tiles), jnp.int32),
        V((groups, width), F32),
        V((groups, width), F32),
        V((groups, width), F32),
        V((1, width), F32),
        V((1, quarter), F32),
        V((1, quarter), F32),
        D((10,)),
        V((tiles, quarter, row_count), BF),
        V((share, nf * quarter, row_count), BF),
        V((width, width), BF),
        V((share, row_count), F32),
        V((tiles, LANES), F32),
        V((groups, width), F32),
        V((tiles, LANES), BF),
        V((share, row_count), jnp.int32),
        V((1, tiles), jnp.int32),
        V((share, LANES), BF),
        V((share, LANES), BF),
        V((2, NY, GRP, half_w), BF),
        V((2, S, 1, S * 2 * NY), F32),
        V((2, S, 1, S * 2 * NY), F32),
        V((S * 2 * NY, S * 2 * NY), BF),
        V((2, tiles, S * 2 * NY), BF),
        V((2, S * 2 * NY, tiles), BF),
        V((2, S * 2 * NY, LANES), BF),
        V((2, LANES, S * 2 * NY), BF),
        V((2, S, 2 * NY, half_w), BF),
        V((2, S, 2 * NY, half_w), BF),
        V((2, nf, HALVES, part_t, half_w), BF),
        V((2, HALVES, nf, part_t, half_w), BF),
        V((2, HALVES, nf, part_t, half_w), BF),
        V((2, nf, HALVES, part_t, half_w), BF),
        V((HALVES, CHAINS * part_t, LANES), F32),
        V((HALVES, CHAINS * part_t, LANES), F32),
        V((HALVES, CHAINS * part_t, LANES), F32),
        V((HALVES, CHAINS * part_t, LANES), BF),
        V((2, S, 2 * NY, half_w), BF),
        V((2, S, 2 * NY, half_w), BF),
        V((S, 2 * NY, LANES), BF),
        V((S, 2 * NY, LANES), BF),
        V((NY, GRP, LANES), BF),
        V((NY, GRP, LANES), BF),
        V((2, NY, GRP, half_w), BF),
        V((2, NY, GRP, half_w), BF),
        V((nf, groups, LANES), F32),
        D(()),
        D(()),
        D((3,)),
        D((3,)),
        D(()),
        D(()),
        D(()),
        D(()),
        D(()),
        D(()),
        D(()),
        D((HALVES,)),
        D(()),
        D(()),
        D(()),
        D(()),
        D(()),
        D(()),
        D(()),
        D(()),
        D(()),
        D(()),
        D(()),
        D(()),
    ]
    vm = pl.BlockSpec(memory_space=pltpu.VMEM)
    shapes = (
        jax.ShapeDtypeStruct((groups, width), F32),
        jax.ShapeDtypeStruct((groups, width), F32),
        jax.ShapeDtypeStruct((groups, width), F32),
        jax.ShapeDtypeStruct((groups, chains), F32),
    )
    results = pl.pallas_call(
        kernel,
        out_shape=tuple(pltpu.VMEM(x.shape, x.dtype) for x in shapes),
        in_specs=[pl.BlockSpec(memory_space=pltpu.HBM)] * 10,
        out_specs=(vm, vm, vm, vm),
        scratch_shapes=scratch,
        compiler_params=pltpu.CompilerParams(collective_id=0, has_side_effects=True),
        name="leapfrog",
    )(
        observations,
        labels,
        tile_live[None, :],
        tile_group[None, :],
        position,
        momentum,
        gradient,
        prior_mean[None, :],
        prior_prec[None, :],
        inv_mass[None, :],
    )
    return pl.pallas_call(
        hand_over,
        out_shape=shapes,
        in_specs=[vm] * 4,
        out_specs=(vm, vm, vm, vm),
        name="hand_over",
    )(*(pltpu.with_memory_space_constraint(x, pltpu.VMEM) for x in results))


def solution(mesh):
    placed = (
        P("dp", "feat", None),
        P("dp", None),
        P("dp"),
        P("dp"),
        P("dp", "feat"),
        P("dp", "feat"),
        P("dp", "feat"),
        P("feat"),
        P("feat"),
        P("feat"),
    )
    return jax.shard_map(
        body,
        mesh=mesh,
        in_specs=placed,
        out_specs=(P("dp", "feat"), P("dp", "feat"), P("dp", "feat"), P("dp", None)),
        check_vma=False,
    )
```

```python
import functools

import jax
import jax.numpy as jnp
from jax import lax
from jax.experimental import pallas as pl
from jax.experimental.pallas import tpu as pltpu
from jax.sharding import PartitionSpec as P

MESH = pl.DeviceIdType.MESH
step_size = 0.1

NY = 8
NC = 2
CHAINS = 16
HALVES = 2
GRP = 16
LANES = 128
BF = jnp.bfloat16
F32 = jnp.float32


def far_first(n):
    return sorted(range(1, n), key=lambda i: -min(i, n - i))


def dot(a, b, contract=((1,), (0,))):
    return lax.dot_general(a, b, (contract, ((), ())), preferred_element_type=F32)


def one_hot(flags):
    return jnp.where(flags, 1.0, 0.0).astype(BF)


def kernel(
    obs,
    lab_h,
    live_h,
    tg_h,
    pos_h,
    mom_h,
    grd_h,
    pm_h,
    pp_h,
    im_h,
    new_pos,
    new_mom,
    new_grd,
    energy,
    lab,
    live,
    tg,
    pos,
    mom,
    grd,
    pm,
    ppim_p,
    ppim_m,
    in_s,
    obs_v,
    obsx,
    perm,
    labf,
    mask,
    half_s,
    ltile,
    lab_r,
    live_r,
    lt_s,
    lt_r,
    gat,
    rqs,
    rq,
    fold,
    tmat,
    tmat_t,
    smat,
    smat_t,
    sels,
    selr,
    xs,
    xr,
    gs,
    gr,
    wf,
    gf,
    lg,
    res,
    ms,
    mr,
    ls,
    lr,
    zs,
    zr,
    ys,
    yr,
    er,
    obs_ss,
    obs_rs,
    lab_ss,
    lab_rs,
    gat_ss,
    gat_rs,
    rq_ss,
    rq_rs,
    sel_ss,
    sel_rs,
    x_ss,
    x_rs,
    gx_ss,
    gx_rs,
    m_ss,
    m_rs,
    l_ss,
    l_rs,
    z_ss,
    z_rs,
    y_ss,
    y_rs,
    e_ss,
    e_rs,
):
    d = lax.axis_index("dp")
    k = lax.axis_index("feat")
    y, z, c = d // (NY * NC), (d // NC) % NY, d % NC
    tiles = lab_h.shape[0]
    nf = 4
    share = tiles // nf
    part_t = share // HALVES
    width = pos_h.shape[1]
    quarter = width // CHAINS
    half_w = width // 2

    def at(yy, zz, cc):
        return ((yy * NY + zz) * NC + cc, k)

    def xpeer(i):
        return (d, (k + i) % nf)

    def xcross(i):
        return (d + 1 - 2 * c, (k + i) % nf)

    g_me = (y, z)
    s_me = (z * NC + c, y * NC + c)

    def g_peer(a, i):
        return at((y + i) % NY, z, c) if a == 0 else at(y, (z + i) % NY, c)

    def s_peer(a, i):
        q = (s_me[a] + i) % (NY * NC)
        return at(y, q // NC, q % NC) if a == 0 else at(q // NC, z, q % NC)

    x_order = (2, 1, 3)
    g_order = far_first(NY)
    x_all = x_order + (0,)
    s_order = far_first(NY * NC)

    barrier = pltpu.get_barrier_semaphore()
    greet = []
    for i in g_order:
        for cc in (c, 1 - c):
            greet += [at((y + i) % NY, z, cc), at(y, (z + i) % NY, cc)]
    greet += [xpeer(i) for i in x_order] + [xcross(i) for i in x_all]
    for who in greet:
        pl.semaphore_signal(barrier, inc=1, device_id=who, device_id_type=MESH)
    count = len(greet)

    loads = []
    for i, (far, near) in enumerate(
        (
            (tg_h, tg),
            (pp_h, ppim_p),
            (im_h, ppim_m),
            (pos_h, pos),
            (mom_h, mom),
            (grd_h, grd),
            (pm_h, pm),
            (live_h, live),
            (lab_h, lab),
            (obs, obs_v),
        )
    ):
        loads.append(pltpu.make_async_copy(far, near, in_s.at[i]))
        loads[-1].start()

    src = lax.broadcasted_iota(jnp.int32, (LANES, width), 0)
    dst = lax.broadcasted_iota(jnp.int32, (LANES, width), 1)
    want = (dst % quarter) * CHAINS + dst // quarter
    for b in range(width // LANES):
        perm[b * LANES : (b + 1) * LANES, :] = one_hot(src + b * LANES == want)

    for copy in loads[1:7]:
        copy.wait()
    row8 = lax.broadcasted_iota(jnp.int32, (8, quarter), 0)
    pieces = jnp.zeros((8, quarter), F32)
    for n, ref in enumerate((ppim_p, ppim_m)):
        rest = ref[...]
        for m in range(3):
            piece = rest.astype(BF).astype(F32)
            pieces = jnp.where(row8 == 3 * n + m, piece, pieces)
            rest = rest - piece
    feature = lax.broadcasted_iota(jnp.int32, (quarter, width), 0)
    chain_lane = lax.broadcasted_iota(jnp.int32, (quarter, width), 1)
    spread = dot(pieces.astype(BF), one_hot(chain_lane // CHAINS == feature))
    pp = (spread[0:1, :] + spread[1:2, :]) + spread[2:3, :]
    im = (spread[3:4, :] + spread[4:5, :]) + spread[5:6, :]

    half = mom[...] - 0.5 * step_size * grd[...]
    moved = pos[...] + step_size * im * half
    half_s[...] = half
    new_pos[...] = moved
    block = dot(moved.astype(BF), perm[...]).astype(BF)
    for a in range(2):
        gat[a, pl.ds(g_me[a], 1)] = block[None, :, a * half_w : (a + 1) * half_w]

    loads[0].wait()
    tile_row = jnp.broadcast_to(tg[...], (tiles, tiles))
    tile_col = jnp.transpose(tile_row.astype(F32)).astype(jnp.int32)
    own_row, own_col = tile_row // GRP, tile_col // GRP
    t_row = lax.broadcasted_iota(jnp.int32, (tiles, tiles), 1)
    t_col = lax.broadcasted_iota(jnp.int32, (tiles, tiles), 0)
    same = own_row == own_col
    rank_row = jnp.sum(jnp.where(same & (t_col < t_row), 1.0, 0.0), axis=0, keepdims=True)
    rank_row = jnp.broadcast_to(rank_row, (tiles, tiles))
    rank_col = jnp.transpose(rank_row).astype(jnp.int32)
    rank_row = rank_row.astype(jnp.int32)
    nq = NY * NC
    slots = nq * NY * 2

    def slot_of(a, own, rank):
        oy, oz, oc = own // (NY * NC), (own // NC) % NY, own % NC
        first, second = (oy, oz) if a == 0 else (oz, oy)
        return (second * NC + oc + nq - s_me[a]) % nq * (NY * 2) + first * 2 + rank, first

    for b in range(slots // LANES):
        here = lax.broadcasted_iota(jnp.int32, (LANES, slots), 0) + b * LANES
        there = lax.broadcasted_iota(jnp.int32, (LANES, slots), 1)
        fold[b * LANES : (b + 1) * LANES, :] = one_hot(here % (NY * 2) == there % (NY * 2))
    lane_q = lax.broadcasted_iota(jnp.int32, (NY * NC, slots), 1) // (NY * 2)
    row_q = lax.broadcasted_iota(jnp.int32, (NY * NC, slots), 0)
    for a in range(2):
        s_r, first = slot_of(a, own_row, rank_row)
        asked = (first * GRP + tile_row % GRP + 1)[:16, :].astype(F32).astype(BF)
        s_c, _ = slot_of(a, own_col, rank_col)
        for b in range(slots // LANES):
            tmat[a, :, b * LANES : (b + 1) * LANES] = one_hot(s_c == t_row + b * LANES)
            tmat_t[a, b * LANES : (b + 1) * LANES, :] = one_hot(s_r == t_col + b * LANES)
        wanted = jnp.broadcast_to(dot(asked, tmat[a])[:1, :], (NY * NC, slots))
        spread_q = dot(jnp.where(lane_q == row_q, wanted, 0.0).astype(BF), fold[...])
        placed = jnp.where(lane_q == (nq - row_q) % nq, spread_q, 0.0)
        for q in range(NY * NC):
            rqs[a, q] = placed[q : q + 1, :]

    pl.semaphore_wait(barrier, count)

    def send(src_ref, dst_ref, ss, rs, who):
        copy = pltpu.make_async_remote_copy(
            src_ref=src_ref, dst_ref=dst_ref, send_sem=ss, recv_sem=rs, device_id=who, device_id_type=MESH
        )
        copy.start()

    def arrived(view, sem):
        pltpu.make_async_copy(view, view, sem).wait()

    for copy in loads[7:]:
        copy.wait()
    mine = pl.ds(pl.multiple_of(k * quarter, quarter), quarter)
    rows = pl.ds(pl.multiple_of(k * share, share), share)
    for i in x_all:
        to = (k + i) % nf
        send(obs_v.at[pl.ds(to * share, share)], obsx.at[:, mine, :], obs_ss, obs_rs, xcross(i))
    send(lab.at[rows], lab_r, lab_ss.at[0], lab_rs.at[0], xcross(0))
    send(live, live_r, lab_ss.at[1], lab_rs.at[1], xcross(0))
    hops = {}
    for i in s_order:
        hops.setdefault(min(i // NC, NY - i // NC), []).append(i)
    for far in sorted(hops, reverse=True):
        for i in hops[far]:
            for a in range(2):
                send(rqs.at[a, i], rq.at[a, nq - i], rq_ss, rq_rs, s_peer(a, i))
        for i in g_order:
            if min(i, NY - i) == far:
                for a in range(2):
                    ref = gat.at[a, g_me[a]]
                    send(ref, ref, gat_ss, gat_rs, g_peer(a, i))
    for a in range(2):
        rq[a, 0] = rqs[a, 0]
    arrived(rq.at[:, pl.ds(0, NY * NC - 1)], rq_rs)
    for a in range(2):
        ask = jnp.sum(rq[a].reshape(NY * NC, slots), axis=0, keepdims=True)
        for b in range(slots // LANES):
            part = jnp.broadcast_to(ask[:, b * LANES : (b + 1) * LANES], (LANES, LANES))
            chosen = jnp.where(part == (t_col + 1).astype(F32), 1.0, 0.0)
            smat_t[a, :, b * LANES : (b + 1) * LANES] = chosen.astype(BF)
            smat[a, b * LANES : (b + 1) * LANES, :] = jnp.transpose(chosen).astype(BF)
    arrived(gat.at[:, pl.ds(0, NY - 1)], gat_rs)
    far_q, near_q = (i for i in s_order if 4 <= i <= 12), (i for i in s_order if not 4 <= i <= 12)
    for span, targets in ((((4, 13),), far_q), (((0, 4), (13, nq)), near_q)):
        for a in range(2):
            table = gat[a].reshape(NY * GRP, half_w)
            for lo, hi in span:
                picked = dot(smat[a, lo * 2 * NY : hi * 2 * NY, :], table).astype(BF)
                sels[a, lo:hi] = picked.reshape(hi - lo, NY * 2, half_w)
        for i in targets:
            for a in range(2):
                send(sels.at[a, i], selr.at[a, nq - i], sel_ss, sel_rs, s_peer(a, i))
    for a in range(2):
        selr[a, 0] = sels[a, 0]

    arrived(lab_r, lab_rs.at[0])
    arrived(live_r, lab_rs.at[1])
    labf[...] = lab_r[...].astype(F32)
    live_col = jnp.transpose(jnp.broadcast_to(live_r[...], (tiles, tiles)).astype(F32))
    mask[...] = jnp.where(t_row.astype(F32) < live_col, 1.0, 0.0)
    ltile[...] = jnp.zeros_like(ltile)

    arrived(selr.at[:, pl.ds(0, NY * NC - 1)], sel_rs)
    for a in range(2):
        rows_a = dot(tmat[a], selr[a].reshape(slots, half_w)).astype(BF)
        xs[a] = rows_a.reshape(nf, HALVES, part_t, half_w)
    for h in range(HALVES):
        for i in x_all:
            for a in range(2):
                to = (k + i) % nf
                send(xs.at[a, to, h], xr.at[a, h, k], x_ss, x_rs.at[h], xcross(i))

    lane = lax.broadcasted_iota(jnp.int32, (part_t, LANES), 1) // quarter
    per = LANES // quarter
    lane16 = lax.broadcasted_iota(jnp.int32, (CHAINS, LANES), 1)
    loglik = jnp.zeros((CHAINS, LANES), F32)
    for h in range(HALVES):
        arrived(xr.at[:, h], x_rs.at[h])
        for a in range(2):
            for b in range(half_w // LANES):
                came = [xr[a, h, kk, :, b * LANES : (b + 1) * LANES].astype(F32) for kk in range(nf)]
                for ci in range(per):
                    out = jnp.zeros((part_t, LANES), F32)
                    for kk in range(nf):
                        shift = ((kk - ci) * quarter) % LANES
                        moved_k = came[kk] if shift == 0 else pltpu.roll(came[kk], shift, 1)
                        out = jnp.where(lane == kk, moved_k, out)
                    chain = a * (CHAINS // 2) + b * per + ci
                    wf[h, chain * part_t : (chain + 1) * part_t, :] = out
        if h == 0:
            arrived(obsx, obs_rs)
        for n in range(part_t):
            coeff = wf[h, pl.ds(n, CHAINS, stride=part_t), :].astype(BF)
            lg[h, n * CHAINS : (n + 1) * CHAINS, :] = dot(coeff, obsx[h * part_t + n])
        for n in range(part_t):
            t = h * part_t + n
            logits = lg[h, n * CHAINS : (n + 1) * CHAINS, :]
            target = jnp.broadcast_to(labf[t : t + 1, :], (CHAINS, LANES))
            alive = jnp.broadcast_to(mask[pl.ds(k * share + t, 1), :], (CHAINS, LANES)) > 0.5
            e = jnp.exp(-jnp.abs(logits))
            r = 1.0 / (1.0 + e)
            sig = jnp.where(logits >= 0.0, r, e * r)
            res[h, n * CHAINS : (n + 1) * CHAINS, :] = jnp.where(alive, sig - target, 0.0).astype(BF)
            soft = jnp.maximum(logits, 0.0) + jnp.log1p(e)
            term = jnp.where(alive, soft - target * logits, 0.0)
            loglik = jnp.where(lane16 == t, jnp.sum(term, axis=1, keepdims=True), loglik)
        for n in range(part_t):
            back = dot(res[h, n * CHAINS : (n + 1) * CHAINS, :], obsx[h * part_t + n], ((1,), (1,)))
            gf[h, pl.ds(n, CHAINS, stride=part_t), :] = back
        for a in range(2):
            for b in range(half_w // LANES):
                chain = a * (CHAINS // 2) + b * per
                made = [gf[h, (chain + ci) * part_t : (chain + ci + 1) * part_t, :] for ci in range(per)]
                for kk in range(nf):
                    out = jnp.zeros((part_t, LANES), F32)
                    for ci in range(per):
                        shift = ((ci - kk) * quarter) % LANES
                        moved_c = made[ci] if shift == 0 else pltpu.roll(made[ci], shift, 1)
                        out = jnp.where(lane == ci, moved_c, out)
                    gs[a, h, kk, :, b * LANES : (b + 1) * LANES] = out.astype(BF)
        for i in x_all:
            for a in range(2):
                to = (k + i) % nf
                send(gs.at[a, h, to], gr.at[a, k, h], gx_ss, gx_rs, xcross(i))

    high = loglik.astype(BF).astype(F32)
    both = jnp.concatenate([high, loglik - high, jnp.zeros((LANES - 2 * CHAINS, LANES), F32)], axis=0)
    lt_s[...] = jnp.transpose(both)[:share, :].astype(BF)
    send(lt_s, lt_r, lab_ss.at[2], lab_rs.at[2], xcross(0))
    arrived(lt_r, lab_rs.at[2])
    ltile[rows, :] = lt_r[...]
    ls[...] = dot(tmat_t[0], ltile[...]).astype(BF).reshape(NY * NC, NY * 2, LANES)
    for i in s_order:
        send(ls.at[i], lr.at[nq - i], l_ss, l_rs, s_peer(0, i))
    lr[0] = ls[0]

    arrived(gr, gx_rs)
    far_q, near_q = (i for i in s_order if 4 <= i <= 12), (i for i in s_order if not 4 <= i <= 12)
    for span, targets in ((((4, 13),), far_q), (((0, 4), (13, nq)), near_q)):
        for a in range(2):
            came = gr[a].reshape(tiles, half_w)
            for lo, hi in span:
                sent = dot(tmat_t[a, lo * 2 * NY : hi * 2 * NY, :], came).astype(BF)
                ms[a, lo:hi] = sent.reshape(hi - lo, NY * 2, half_w)
        for i in targets:
            for a in range(2):
                send(ms.at[a, i], mr.at[a, nq - i], m_ss, m_rs, s_peer(a, i))
    for a in range(2):
        mr[a, 0] = ms[a, 0]

    arrived(lr.at[pl.ds(0, NY * NC - 1)], l_rs)
    zs[...] = dot(smat_t[0], lr[...].reshape(slots, LANES)).astype(BF).reshape(NY, GRP, LANES)
    for i in g_order:
        to = (g_me[0] + i) % NY
        send(zs.at[to], zr.at[g_me[0]], z_ss, z_rs, g_peer(0, i))
    zr[pl.ds(g_me[0], 1)] = zs[pl.ds(g_me[0], 1)]

    offset = new_pos[...] - pm[...]
    prior_term = pp * offset
    prior_quad = prior_term * offset

    arrived(mr.at[:, pl.ds(0, NY * NC - 1)], m_rs)
    for a in range(2):
        summed = dot(smat_t[a], mr[a].reshape(slots, half_w)).astype(BF)
        ys[a] = summed.reshape(NY, GRP, half_w)
    for i in g_order:
        for a in range(2):
            to = (g_me[a] + i) % NY
            send(ys.at[a, to], yr.at[a, g_me[a]], y_ss, y_rs, g_peer(a, i))
    for a in range(2):
        yr[a, pl.ds(g_me[a], 1)] = ys[a, pl.ds(g_me[a], 1)]

    lik = jnp.zeros((GRP, width), F32)
    group_loglik = jnp.zeros((GRP, LANES), F32)
    arrived(zr.at[pl.ds(0, NY - 1)], z_rs)
    for g in range(NY):
        group_loglik = group_loglik + zr[g].astype(F32)
    group_loglik = group_loglik + pltpu.roll(group_loglik, LANES - CHAINS, 1)
    arrived(yr.at[:, pl.ds(0, NY - 1)], y_rs)
    for a in range(2):
        part = yr[a].reshape(NY * GRP, half_w)
        back = dot(part, perm[:, a * half_w : (a + 1) * half_w], ((1,), (1,)))
        for g in range(NY):
            lik = lik + back[g * GRP : (g + 1) * GRP, :]

    grad_now = lik + prior_term
    mom_now = half_s[...] - 0.5 * step_size * grad_now
    quad = 0.5 * (prior_quad + im * mom_now * mom_now)
    total = quad[:, :LANES]
    for b in range(1, width // LANES):
        total = total + quad[:, b * LANES : (b + 1) * LANES]
    shift = LANES // 2
    while shift >= CHAINS:
        total = total + pltpu.roll(total, shift, 1)
        shift //= 2
    total = total + group_loglik
    er[pl.ds(k, 1)] = total[None]
    for i in x_order:
        send(er.at[k], er.at[k], e_ss, e_rs, xpeer(i))
    new_grd[...] = grad_now
    new_mom[...] = mom_now
    for view, sem in (
        (obs_v, obs_ss),
        (rq.at[:, pl.ds(0, NY * NC - 1)], rq_ss),
        (gat.at[:, pl.ds(0, NY - 1)], gat_ss),
        (sels.at[:, pl.ds(0, NY * NC - 1)], sel_ss),
        (xs, x_ss),
        (gs, gx_ss),
        (ls.at[pl.ds(0, NY * NC - 1)], l_ss),
        (ms.at[:, pl.ds(0, NY * NC - 1)], m_ss),
        (zs.at[pl.ds(0, NY - 1)], z_ss),
        (ys.at[:, pl.ds(0, NY - 1)], y_ss),
        (lab_r, lab_ss.at[0]),
        (live_r, lab_ss.at[1]),
        (lt_s, lab_ss.at[2]),
    ):
        arrived(view, sem)
    arrived(er.at[pl.ds(0, nf - 1)], e_rs)
    whole = er[0]
    for kk in range(1, nf):
        whole = whole + er[kk]
    energy[...] = whole[:, :CHAINS]
    arrived(er.at[pl.ds(0, nf - 1)], e_ss)


def hand_over(a, b, c, d, a_out, b_out, c_out, d_out):
    a_out[...] = a[...]
    b_out[...] = b[...]
    c_out[...] = c[...]
    d_out[...] = d[...]


def body(observations, labels, tile_live, tile_group, position, momentum, gradient, prior_mean, prior_prec, inv_mass):
    tiles, quarter, row_count = observations.shape
    groups, width = position.shape
    chains = width // quarter
    nf = lax.axis_size("feat")
    half_w = width // 2
    share = tiles // nf
    S = NY * NC
    part_t = share // HALVES
    V = pltpu.VMEM
    D = pltpu.SemaphoreType.DMA
    S = NY * NC
    scratch = [
        V((tiles, row_count), jnp.int32),
        V((1, tiles), jnp.int32),
        V((1, tiles), jnp.int32),
        V((groups, width), F32),
        V((groups, width), F32),
        V((groups, width), F32),
        V((1, width), F32),
        V((1, quarter), F32),
        V((1, quarter), F32),
        D((10,)),
        V((tiles, quarter, row_count), BF),
        V((share, nf * quarter, row_count), BF),
        V((width, width), BF),
        V((share, row_count), F32),
        V((tiles, LANES), F32),
        V((groups, width), F32),
        V((tiles, LANES), BF),
        V((share, row_count), jnp.int32),
        V((1, tiles), jnp.int32),
        V((share, LANES), BF),
        V((share, LANES), BF),
        V((2, NY, GRP, half_w), BF),
        V((2, S, 1, S * 2 * NY), F32),
        V((2, S, 1, S * 2 * NY), F32),
        V((S * 2 * NY, S * 2 * NY), BF),
        V((2, tiles, S * 2 * NY), BF),
        V((2, S * 2 * NY, tiles), BF),
        V((2, S * 2 * NY, LANES), BF),
        V((2, LANES, S * 2 * NY), BF),
        V((2, S, 2 * NY, half_w), BF),
        V((2, S, 2 * NY, half_w), BF),
        V((2, nf, HALVES, part_t, half_w), BF),
        V((2, HALVES, nf, part_t, half_w), BF),
        V((2, HALVES, nf, part_t, half_w), BF),
        V((2, nf, HALVES, part_t, half_w), BF),
        V((HALVES, CHAINS * part_t, LANES), F32),
        V((HALVES, CHAINS * part_t, LANES), F32),
        V((HALVES, CHAINS * part_t, LANES), F32),
        V((HALVES, CHAINS * part_t, LANES), BF),
        V((2, S, 2 * NY, half_w), BF),
        V((2, S, 2 * NY, half_w), BF),
        V((S, 2 * NY, LANES), BF),
        V((S, 2 * NY, LANES), BF),
        V((NY, GRP, LANES), BF),
        V((NY, GRP, LANES), BF),
        V((2, NY, GRP, half_w), BF),
        V((2, NY, GRP, half_w), BF),
        V((nf, groups, LANES), F32),
        D(()),
        D(()),
        D((3,)),
        D((3,)),
        D(()),
        D(()),
        D(()),
        D(()),
        D(()),
        D(()),
        D(()),
        D((HALVES,)),
        D(()),
        D(()),
        D(()),
        D(()),
        D(()),
        D(()),
        D(()),
        D(()),
        D(()),
        D(()),
        D(()),
        D(()),
    ]
    vm = pl.BlockSpec(memory_space=pltpu.VMEM)
    shapes = (
        jax.ShapeDtypeStruct((groups, width), F32),
        jax.ShapeDtypeStruct((groups, width), F32),
        jax.ShapeDtypeStruct((groups, width), F32),
        jax.ShapeDtypeStruct((groups, chains), F32),
    )
    results = pl.pallas_call(
        kernel,
        out_shape=tuple(pltpu.VMEM(x.shape, x.dtype) for x in shapes),
        in_specs=[pl.BlockSpec(memory_space=pltpu.HBM)] * 10,
        out_specs=(vm, vm, vm, vm),
        scratch_shapes=scratch,
        compiler_params=pltpu.CompilerParams(collective_id=0, has_side_effects=True),
        name="leapfrog",
    )(
        observations,
        labels,
        tile_live[None, :],
        tile_group[None, :],
        position,
        momentum,
        gradient,
        prior_mean[None, :],
        prior_prec[None, :],
        inv_mass[None, :],
    )
    return pl.pallas_call(
        hand_over,
        out_shape=shapes,
        in_specs=[vm] * 4,
        out_specs=(vm, vm, vm, vm),
        name="hand_over",
    )(*(pltpu.with_memory_space_constraint(x, pltpu.VMEM) for x in results))


def solution(mesh):
    placed = (
        P("dp", "feat", None),
        P("dp", None),
        P("dp"),
        P("dp"),
        P("dp", "feat"),
        P("dp", "feat"),
        P("dp", "feat"),
        P("feat"),
        P("feat"),
        P("feat"),
    )
    return jax.shard_map(
        body,
        mesh=mesh,
        in_specs=placed,
        out_specs=(P("dp", "feat"), P("dp", "feat"), P("dp", "feat"), P("dp", None)),
        check_vma=False,
    )
```

```python
import functools

import jax
import jax.numpy as jnp
from jax import lax
from jax.experimental import pallas as pl
from jax.experimental.pallas import tpu as pltpu
from jax.sharding import PartitionSpec as P

MESH = pl.DeviceIdType.MESH
step_size = 0.1

NY = 8
NC = 2
CHAINS = 16
HALVES = 2
GRP = 16
LANES = 128
BF = jnp.bfloat16
F32 = jnp.float32


def far_first(n):
    return sorted(range(1, n), key=lambda i: -min(i, n - i))


def dot(a, b, contract=((1,), (0,))):
    return lax.dot_general(a, b, (contract, ((), ())), preferred_element_type=F32)


def one_hot(flags):
    return jnp.where(flags, 1.0, 0.0).astype(BF)


def kernel(
    obs,
    lab_h,
    live_h,
    tg_h,
    pos_h,
    mom_h,
    grd_h,
    pm_h,
    pp_h,
    im_h,
    new_pos,
    new_mom,
    new_grd,
    energy,
    lab,
    live,
    tg,
    pos,
    mom,
    grd,
    pm,
    ppim_p,
    ppim_m,
    in_s,
    obs_v,
    obsx,
    perm,
    labf,
    mask,
    half_s,
    ltile,
    lab_r,
    live_r,
    lt_s,
    lt_r,
    gat,
    rqs,
    rq,
    fold,
    tmat,
    tmat_t,
    smat,
    smat_t,
    sels,
    selr,
    xs,
    xr,
    gs,
    gr,
    wf,
    gf,
    lg,
    res,
    ms,
    mr,
    ls,
    lr,
    zs,
    zr,
    ys,
    yr,
    er,
    obs_ss,
    obs_rs,
    lab_ss,
    lab_rs,
    gat_ss,
    gat_rs,
    rq_ss,
    rq_rs,
    sel_ss,
    sel_rs,
    x_ss,
    x_rs,
    gx_ss,
    gx_rs,
    m_ss,
    m_rs,
    l_ss,
    l_rs,
    z_ss,
    z_rs,
    y_ss,
    y_rs,
    e_ss,
    e_rs,
):
    d = lax.axis_index("dp")
    k = lax.axis_index("feat")
    y, z, c = d // (NY * NC), (d // NC) % NY, d % NC
    tiles = lab_h.shape[0]
    nf = 4
    share = tiles // nf
    part_t = share // HALVES
    width = pos_h.shape[1]
    quarter = width // CHAINS
    half_w = width // 2

    def at(yy, zz, cc):
        return ((yy * NY + zz) * NC + cc, k)

    def xpeer(i):
        return (d, (k + i) % nf)

    def xcross(i):
        return (d + 1 - 2 * c, (k + i) % nf)

    g_me = (y, z)
    s_me = (z * NC + c, y * NC + c)

    def g_peer(a, i):
        return at((y + i) % NY, z, c) if a == 0 else at(y, (z + i) % NY, c)

    def s_peer(a, i):
        q = (s_me[a] + i) % (NY * NC)
        return at(y, q // NC, q % NC) if a == 0 else at(q // NC, z, q % NC)

    x_order = (2, 1, 3)
    g_order = far_first(NY)
    x_all = x_order + (0,)
    s_order = far_first(NY * NC)

    barrier = pltpu.get_barrier_semaphore()
    greet = []
    for i in g_order:
        for cc in (c, 1 - c):
            greet += [at((y + i) % NY, z, cc), at(y, (z + i) % NY, cc)]
    greet += [xpeer(i) for i in x_order] + [xcross(i) for i in x_all]
    for who in greet:
        pl.semaphore_signal(barrier, inc=1, device_id=who, device_id_type=MESH)
    count = len(greet)

    loads = []
    for i, (far, near) in enumerate(
        (
            (tg_h, tg),
            (pp_h, ppim_p),
            (im_h, ppim_m),
            (pos_h, pos),
            (mom_h, mom),
            (grd_h, grd),
            (pm_h, pm),
            (live_h, live),
            (lab_h, lab),
            (obs, obs_v),
        )
    ):
        loads.append(pltpu.make_async_copy(far, near, in_s.at[i]))
        loads[-1].start()

    src = lax.broadcasted_iota(jnp.int32, (LANES, width), 0)
    dst = lax.broadcasted_iota(jnp.int32, (LANES, width), 1)
    want = (dst % quarter) * CHAINS + dst // quarter
    for b in range(width // LANES):
        perm[b * LANES : (b + 1) * LANES, :] = one_hot(src + b * LANES == want)

    for copy in loads[1:7]:
        copy.wait()
    row8 = lax.broadcasted_iota(jnp.int32, (8, quarter), 0)
    pieces = jnp.zeros((8, quarter), F32)
    for n, ref in enumerate((ppim_p, ppim_m)):
        rest = ref[...]
        for m in range(3):
            piece = rest.astype(BF).astype(F32)
            pieces = jnp.where(row8 == 3 * n + m, piece, pieces)
            rest = rest - piece
    feature = lax.broadcasted_iota(jnp.int32, (quarter, width), 0)
    chain_lane = lax.broadcasted_iota(jnp.int32, (quarter, width), 1)
    spread = dot(pieces.astype(BF), one_hot(chain_lane // CHAINS == feature))
    pp = (spread[0:1, :] + spread[1:2, :]) + spread[2:3, :]
    im = (spread[3:4, :] + spread[4:5, :]) + spread[5:6, :]

    half = mom[...] - 0.5 * step_size * grd[...]
    moved = pos[...] + step_size * im * half
    half_s[...] = half
    new_pos[...] = moved
    block = dot(moved.astype(BF), perm[...]).astype(BF)
    for a in range(2):
        gat[a, 0] = block[:, a * half_w : (a + 1) * half_w]

    loads[0].wait()
    tile_row = jnp.broadcast_to(tg[...], (tiles, tiles))
    tile_col = jnp.transpose(tile_row.astype(F32)).astype(jnp.int32)
    own_row, own_col = tile_row // GRP, tile_col // GRP
    t_row = lax.broadcasted_iota(jnp.int32, (tiles, tiles), 1)
    t_col = lax.broadcasted_iota(jnp.int32, (tiles, tiles), 0)
    same = own_row == own_col
    rank_row = jnp.sum(jnp.where(same & (t_col < t_row), 1.0, 0.0), axis=0, keepdims=True)
    rank_row = jnp.broadcast_to(rank_row, (tiles, tiles))
    rank_col = jnp.transpose(rank_row).astype(jnp.int32)
    rank_row = rank_row.astype(jnp.int32)
    nq = NY * NC
    slots = nq * NY * 2

    def slot_of(a, own, rank):
        oy, oz, oc = own // (NY * NC), (own // NC) % NY, own % NC
        first, second = (oy, oz) if a == 0 else (oz, oy)
        return (second * NC + oc + nq - s_me[a]) % nq * (NY * 2) + first * 2 + rank, first

    for b in range(slots // LANES):
        here = lax.broadcasted_iota(jnp.int32, (LANES, slots), 0) + b * LANES
        there = lax.broadcasted_iota(jnp.int32, (LANES, slots), 1)
        fold[b * LANES : (b + 1) * LANES, :] = one_hot(here % (NY * 2) == there % (NY * 2))
    lane_q = lax.broadcasted_iota(jnp.int32, (NY * NC, slots), 1) // (NY * 2)
    row_q = lax.broadcasted_iota(jnp.int32, (NY * NC, slots), 0)
    for a in range(2):
        s_r, first = slot_of(a, own_row, rank_row)
        asked = ((first + NY - g_me[a]) % NY * GRP + tile_row % GRP + 1)[:16, :].astype(F32).astype(BF)
        s_c, _ = slot_of(a, own_col, rank_col)
        for b in range(slots // LANES):
            tmat[a, :, b * LANES : (b + 1) * LANES] = one_hot(s_c == t_row + b * LANES)
            tmat_t[a, b * LANES : (b + 1) * LANES, :] = one_hot(s_r == t_col + b * LANES)
        wanted = jnp.broadcast_to(dot(asked, tmat[a])[:1, :], (NY * NC, slots))
        spread_q = dot(jnp.where(lane_q == row_q, wanted, 0.0).astype(BF), fold[...])
        placed = jnp.where(lane_q == (nq - row_q) % nq, spread_q, 0.0)
        for q in range(NY * NC):
            rqs[a, q] = placed[q : q + 1, :]

    pl.semaphore_wait(barrier, count)

    def send(src_ref, dst_ref, ss, rs, who):
        copy = pltpu.make_async_remote_copy(
            src_ref=src_ref, dst_ref=dst_ref, send_sem=ss, recv_sem=rs, device_id=who, device_id_type=MESH
        )
        copy.start()

    def arrived(view, sem):
        pltpu.make_async_copy(view, view, sem).wait()

    for copy in loads[7:]:
        copy.wait()
    mine = pl.ds(pl.multiple_of(k * quarter, quarter), quarter)
    rows = pl.ds(pl.multiple_of(k * share, share), share)
    for i in x_all:
        to = (k + i) % nf
        send(obs_v.at[pl.ds(to * share, share)], obsx.at[:, mine, :], obs_ss, obs_rs, xcross(i))
    send(lab.at[rows], lab_r, lab_ss.at[0], lab_rs.at[0], xcross(0))
    send(live, live_r, lab_ss.at[1], lab_rs.at[1], xcross(0))
    hops = {}
    for i in s_order:
        hops.setdefault(min(i // NC, NY - i // NC), []).append(i)
    for far in sorted(hops, reverse=True):
        for i in hops[far]:
            for a in range(2):
                send(rqs.at[a, i], rq.at[a, nq - i], rq_ss, rq_rs, s_peer(a, i))
        for i in g_order:
            if min(i, NY - i) == far:
                for a in range(2):
                    send(gat.at[a, 0], gat.at[a, NY - i], gat_ss, gat_rs, g_peer(a, i))
    for a in range(2):
        rq[a, 0] = rqs[a, 0]
    arrived(rq.at[:, pl.ds(0, NY * NC - 1)], rq_rs)
    for a in range(2):
        ask = jnp.sum(rq[a].reshape(NY * NC, slots), axis=0, keepdims=True)
        for b in range(slots // LANES):
            part = jnp.broadcast_to(ask[:, b * LANES : (b + 1) * LANES], (LANES, LANES))
            chosen = jnp.where(part == (t_col + 1).astype(F32), 1.0, 0.0)
            smat_t[a, :, b * LANES : (b + 1) * LANES] = chosen.astype(BF)
            smat[a, b * LANES : (b + 1) * LANES, :] = jnp.transpose(chosen).astype(BF)
    arrived(gat.at[:, pl.ds(0, NY - 1)], gat_rs)
    far_q, near_q = (i for i in s_order if 4 <= i <= 12), (i for i in s_order if not 4 <= i <= 12)
    for span, targets in ((((4, 13),), far_q), (((0, 4), (13, nq)), near_q)):
        for a in range(2):
            table = gat[a].reshape(NY * GRP, half_w)
            for lo, hi in span:
                picked = dot(smat[a, lo * 2 * NY : hi * 2 * NY, :], table).astype(BF)
                sels[a, lo:hi] = picked.reshape(hi - lo, NY * 2, half_w)
        for i in targets:
            for a in range(2):
                send(sels.at[a, i], selr.at[a, nq - i], sel_ss, sel_rs, s_peer(a, i))
    for a in range(2):
        selr[a, 0] = sels[a, 0]

    arrived(lab_r, lab_rs.at[0])
    arrived(live_r, lab_rs.at[1])
    labf[...] = lab_r[...].astype(F32)
    live_col = jnp.transpose(jnp.broadcast_to(live_r[...], (tiles, tiles)).astype(F32))
    mask[...] = jnp.where(t_row.astype(F32) < live_col, 1.0, 0.0)
    ltile[...] = jnp.zeros_like(ltile)

    arrived(selr.at[:, pl.ds(0, NY * NC - 1)], sel_rs)
    for a in range(2):
        rows_a = dot(tmat[a], selr[a].reshape(slots, half_w)).astype(BF)
        xs[a] = rows_a.reshape(nf, HALVES, part_t, half_w)
    for h in range(HALVES):
        for i in x_all:
            for a in range(2):
                to = (k + i) % nf
                send(xs.at[a, to, h], xr.at[a, h, k], x_ss, x_rs.at[h], xcross(i))

    lane = lax.broadcasted_iota(jnp.int32, (part_t, LANES), 1) // quarter
    per = LANES // quarter
    lane16 = lax.broadcasted_iota(jnp.int32, (CHAINS, LANES), 1)
    loglik = jnp.zeros((CHAINS, LANES), F32)
    for h in range(HALVES):
        arrived(xr.at[:, h], x_rs.at[h])
        for a in range(2):
            for b in range(half_w // LANES):
                came = [xr[a, h, kk, :, b * LANES : (b + 1) * LANES].astype(F32) for kk in range(nf)]
                for ci in range(per):
                    out = jnp.zeros((part_t, LANES), F32)
                    for kk in range(nf):
                        shift = ((kk - ci) * quarter) % LANES
                        moved_k = came[kk] if shift == 0 else pltpu.roll(came[kk], shift, 1)
                        out = jnp.where(lane == kk, moved_k, out)
                    chain = a * (CHAINS // 2) + b * per + ci
                    wf[h, chain * part_t : (chain + 1) * part_t, :] = out
        if h == 0:
            arrived(obsx, obs_rs)
        for n in range(part_t):
            coeff = wf[h, pl.ds(n, CHAINS, stride=part_t), :].astype(BF)
            lg[h, n * CHAINS : (n + 1) * CHAINS, :] = dot(coeff, obsx[h * part_t + n])
        for n in range(part_t):
            t = h * part_t + n
            logits = lg[h, n * CHAINS : (n + 1) * CHAINS, :]
            target = jnp.broadcast_to(labf[t : t + 1, :], (CHAINS, LANES))
            alive = jnp.broadcast_to(mask[pl.ds(k * share + t, 1), :], (CHAINS, LANES)) > 0.5
            e = jnp.exp(-jnp.abs(logits))
            r = 1.0 / (1.0 + e)
            sig = jnp.where(logits >= 0.0, r, e * r)
            res[h, n * CHAINS : (n + 1) * CHAINS, :] = jnp.where(alive, sig - target, 0.0).astype(BF)
            soft = jnp.maximum(logits, 0.0) + jnp.log1p(e)
            term = jnp.where(alive, soft - target * logits, 0.0)
            loglik = jnp.where(lane16 == t, jnp.sum(term, axis=1, keepdims=True), loglik)
        for n in range(part_t):
            back = dot(res[h, n * CHAINS : (n + 1) * CHAINS, :], obsx[h * part_t + n], ((1,), (1,)))
            gf[h, pl.ds(n, CHAINS, stride=part_t), :] = back
        for a in range(2):
            for b in range(half_w // LANES):
                chain = a * (CHAINS // 2) + b * per
                made = [gf[h, (chain + ci) * part_t : (chain + ci + 1) * part_t, :] for ci in range(per)]
                for kk in range(nf):
                    out = jnp.zeros((part_t, LANES), F32)
                    for ci in range(per):
                        shift = ((ci - kk) * quarter) % LANES
                        moved_c = made[ci] if shift == 0 else pltpu.roll(made[ci], shift, 1)
                        out = jnp.where(lane == ci, moved_c, out)
                    gs[a, h, kk, :, b * LANES : (b + 1) * LANES] = out.astype(BF)
        for i in x_all:
            for a in range(2):
                to = (k + i) % nf
                send(gs.at[a, h, to], gr.at[a, k, h], gx_ss, gx_rs, xcross(i))

    high = loglik.astype(BF).astype(F32)
    both = jnp.concatenate([high, loglik - high, jnp.zeros((LANES - 2 * CHAINS, LANES), F32)], axis=0)
    lt_s[...] = jnp.transpose(both)[:share, :].astype(BF)
    send(lt_s, lt_r, lab_ss.at[2], lab_rs.at[2], xcross(0))
    arrived(lt_r, lab_rs.at[2])
    ltile[rows, :] = lt_r[...]
    ls[...] = dot(tmat_t[0], ltile[...]).astype(BF).reshape(NY * NC, NY * 2, LANES)
    for i in s_order:
        send(ls.at[i], lr.at[nq - i], l_ss, l_rs, s_peer(0, i))
    lr[0] = ls[0]

    arrived(gr, gx_rs)
    far_q, near_q = (i for i in s_order if 4 <= i <= 12), (i for i in s_order if not 4 <= i <= 12)
    for span, targets in ((((4, 13),), far_q), (((0, 4), (13, nq)), near_q)):
        for a in range(2):
            came = gr[a].reshape(tiles, half_w)
            for lo, hi in span:
                sent = dot(tmat_t[a, lo * 2 * NY : hi * 2 * NY, :], came).astype(BF)
                ms[a, lo:hi] = sent.reshape(hi - lo, NY * 2, half_w)
        for i in targets:
            for a in range(2):
                send(ms.at[a, i], mr.at[a, nq - i], m_ss, m_rs, s_peer(a, i))
    for a in range(2):
        mr[a, 0] = ms[a, 0]

    arrived(lr.at[pl.ds(0, NY * NC - 1)], l_rs)
    zs[...] = dot(smat_t[0], lr[...].reshape(slots, LANES)).astype(BF).reshape(NY, GRP, LANES)
    for i in g_order:
        send(zs.at[i], zr.at[NY - i], z_ss, z_rs, g_peer(0, i))
    zr[0] = zs[0]

    offset = new_pos[...] - pm[...]
    prior_term = pp * offset
    prior_quad = prior_term * offset

    arrived(mr.at[:, pl.ds(0, NY * NC - 1)], m_rs)
    for span, near in ((((2, 7),), False), (((0, 2), (7, NY)), True)):
        for a in range(2):
            came = mr[a].reshape(slots, half_w)
            for lo, hi in span:
                summed = dot(smat_t[a, lo * GRP : hi * GRP, :], came).astype(BF)
                ys[a, lo:hi] = summed.reshape(hi - lo, GRP, half_w)
        for i in g_order:
            if (min(i, NY - i) == 1) == near:
                for a in range(2):
                    send(ys.at[a, i], yr.at[a, NY - i], y_ss, y_rs, g_peer(a, i))
    for a in range(2):
        yr[a, 0] = ys[a, 0]

    lik = jnp.zeros((GRP, width), F32)
    group_loglik = jnp.zeros((GRP, LANES), F32)
    arrived(zr.at[pl.ds(0, NY - 1)], z_rs)
    for g in range(NY):
        group_loglik = group_loglik + zr[g].astype(F32)
    group_loglik = group_loglik + pltpu.roll(group_loglik, LANES - CHAINS, 1)
    arrived(yr.at[:, pl.ds(0, NY - 1)], y_rs)
    for a in range(2):
        part = yr[a].reshape(NY * GRP, half_w)
        back = dot(part, perm[:, a * half_w : (a + 1) * half_w], ((1,), (1,)))
        for g in range(NY):
            lik = lik + back[g * GRP : (g + 1) * GRP, :]

    grad_now = lik + prior_term
    mom_now = half_s[...] - 0.5 * step_size * grad_now
    quad = 0.5 * (prior_quad + im * mom_now * mom_now)
    total = quad[:, :LANES]
    for b in range(1, width // LANES):
        total = total + quad[:, b * LANES : (b + 1) * LANES]
    shift = LANES // 2
    while shift >= CHAINS:
        total = total + pltpu.roll(total, shift, 1)
        shift //= 2
    total = total + group_loglik
    er[pl.ds(k, 1)] = total[None]
    for i in x_order:
        send(er.at[k], er.at[k], e_ss, e_rs, xpeer(i))
    new_grd[...] = grad_now
    new_mom[...] = mom_now
    for view, sem in (
        (obs_v, obs_ss),
        (rq.at[:, pl.ds(0, NY * NC - 1)], rq_ss),
        (gat.at[:, pl.ds(0, NY - 1)], gat_ss),
        (sels.at[:, pl.ds(0, NY * NC - 1)], sel_ss),
        (xs, x_ss),
        (gs, gx_ss),
        (ls.at[pl.ds(0, NY * NC - 1)], l_ss),
        (ms.at[:, pl.ds(0, NY * NC - 1)], m_ss),
        (zs.at[pl.ds(0, NY - 1)], z_ss),
        (ys.at[:, pl.ds(0, NY - 1)], y_ss),
        (lab_r, lab_ss.at[0]),
        (live_r, lab_ss.at[1]),
        (lt_s, lab_ss.at[2]),
    ):
        arrived(view, sem)
    arrived(er.at[pl.ds(0, nf - 1)], e_rs)
    whole = er[0]
    for kk in range(1, nf):
        whole = whole + er[kk]
    energy[...] = whole[:, :CHAINS]
    arrived(er.at[pl.ds(0, nf - 1)], e_ss)


def hand_over(a, b, c, d, a_out, b_out, c_out, d_out):
    a_out[...] = a[...]
    b_out[...] = b[...]
    c_out[...] = c[...]
    d_out[...] = d[...]


def body(observations, labels, tile_live, tile_group, position, momentum, gradient, prior_mean, prior_prec, inv_mass):
    tiles, quarter, row_count = observations.shape
    groups, width = position.shape
    chains = width // quarter
    nf = lax.axis_size("feat")
    half_w = width // 2
    share = tiles // nf
    S = NY * NC
    part_t = share // HALVES
    V = pltpu.VMEM
    D = pltpu.SemaphoreType.DMA
    S = NY * NC
    scratch = [
        V((tiles, row_count), jnp.int32),
        V((1, tiles), jnp.int32),
        V((1, tiles), jnp.int32),
        V((groups, width), F32),
        V((groups, width), F32),
        V((groups, width), F32),
        V((1, width), F32),
        V((1, quarter), F32),
        V((1, quarter), F32),
        D((10,)),
        V((tiles, quarter, row_count), BF),
        V((share, nf * quarter, row_count), BF),
        V((width, width), BF),
        V((share, row_count), F32),
        V((tiles, LANES), F32),
        V((groups, width), F32),
        V((tiles, LANES), BF),
        V((share, row_count), jnp.int32),
        V((1, tiles), jnp.int32),
        V((share, LANES), BF),
        V((share, LANES), BF),
        V((2, NY, GRP, half_w), BF),
        V((2, S, 1, S * 2 * NY), F32),
        V((2, S, 1, S * 2 * NY), F32),
        V((S * 2 * NY, S * 2 * NY), BF),
        V((2, tiles, S * 2 * NY), BF),
        V((2, S * 2 * NY, tiles), BF),
        V((2, S * 2 * NY, LANES), BF),
        V((2, LANES, S * 2 * NY), BF),
        V((2, S, 2 * NY, half_w), BF),
        V((2, S, 2 * NY, half_w), BF),
        V((2, nf, HALVES, part_t, half_w), BF),
        V((2, HALVES, nf, part_t, half_w), BF),
        V((2, HALVES, nf, part_t, half_w), BF),
        V((2, nf, HALVES, part_t, half_w), BF),
        V((HALVES, CHAINS * part_t, LANES), F32),
        V((HALVES, CHAINS * part_t, LANES), F32),
        V((HALVES, CHAINS * part_t, LANES), F32),
        V((HALVES, CHAINS * part_t, LANES), BF),
        V((2, S, 2 * NY, half_w), BF),
        V((2, S, 2 * NY, half_w), BF),
        V((S, 2 * NY, LANES), BF),
        V((S, 2 * NY, LANES), BF),
        V((NY, GRP, LANES), BF),
        V((NY, GRP, LANES), BF),
        V((2, NY, GRP, half_w), BF),
        V((2, NY, GRP, half_w), BF),
        V((nf, groups, LANES), F32),
        D(()),
        D(()),
        D((3,)),
        D((3,)),
        D(()),
        D(()),
        D(()),
        D(()),
        D(()),
        D(()),
        D(()),
        D((HALVES,)),
        D(()),
        D(()),
        D(()),
        D(()),
        D(()),
        D(()),
        D(()),
        D(()),
        D(()),
        D(()),
        D(()),
        D(()),
    ]
    vm = pl.BlockSpec(memory_space=pltpu.VMEM)
    shapes = (
        jax.ShapeDtypeStruct((groups, width), F32),
        jax.ShapeDtypeStruct((groups, width), F32),
        jax.ShapeDtypeStruct((groups, width), F32),
        jax.ShapeDtypeStruct((groups, chains), F32),
    )
    results = pl.pallas_call(
        kernel,
        out_shape=tuple(pltpu.VMEM(x.shape, x.dtype) for x in shapes),
        in_specs=[pl.BlockSpec(memory_space=pltpu.HBM)] * 10,
        out_specs=(vm, vm, vm, vm),
        scratch_shapes=scratch,
        compiler_params=pltpu.CompilerParams(collective_id=0, has_side_effects=True),
        name="leapfrog",
    )(
        observations,
        labels,
        tile_live[None, :],
        tile_group[None, :],
        position,
        momentum,
        gradient,
        prior_mean[None, :],
        prior_prec[None, :],
        inv_mass[None, :],
    )
    return pl.pallas_call(
        hand_over,
        out_shape=shapes,
        in_specs=[vm] * 4,
        out_specs=(vm, vm, vm, vm),
        name="hand_over",
    )(*(pltpu.with_memory_space_constraint(x, pltpu.VMEM) for x in results))


def solution(mesh):
    placed = (
        P("dp", "feat", None),
        P("dp", None),
        P("dp"),
        P("dp"),
        P("dp", "feat"),
        P("dp", "feat"),
        P("dp", "feat"),
        P("feat"),
        P("feat"),
        P("feat"),
    )
    return jax.shard_map(
        body,
        mesh=mesh,
        in_specs=placed,
        out_specs=(P("dp", "feat"), P("dp", "feat"), P("dp", "feat"), P("dp", None)),
        check_vma=False,
    )
```
